256 devices in a mesh: dp: 16 (over z, core), row: 8 (over x_lo, y), col: 2 (over x_hi).
Axes of the slice: x: 4 (x_hi: 2, x_lo: 2; x = x_hi * 2 + x_lo), y: 4, z: 8, core: 2. Of those that a mesh axis runs over, the one named last changes fastest.
Arguments:
- patches: bfloat16 [32768, 1408], P(('dp', 'row', 'col')), may hold values from -6 to 6
- norm_gain: float32 [1408], replicated, may hold values from 0.5 to 1.5
- norm_bias: float32 [1408], replicated, may hold values from -3 to 3
- up_weight: bfloat16 [1408, 6144], P('col', 'row'), may hold values from -0.15625 to 0.15625
- up_bias: float32 [6144], P('row'), may hold values from -3 to 3
- down_weight: bfloat16 [6144, 1408], P('row', 'col'), may hold values from -0.078125 to 0.078125
- down_bias: float32 [1408], replicated, may hold values from -3 to 3
- cotangent: bfloat16 [32768, 1408], P(('dp', 'row', 'col')), may hold values from -24 to 24
Outputs:
- output: float32 [32768, 1408], P(('dp', 'row', 'col'))
- patch_grad: float32 [32768, 1408], P(('dp', 'row', 'col'))
- up_grad: float32 [1408, 6144], P('col', 'row')
- down_grad: float32 [6144, 1408], P('row', 'col')
- bias_grad: float32 [6144], P('row')
- norm_grad: float32 [2, 1408], replicated
The draws below stay inside these ranges and needn't reach their ends.
All inputs are finite; a program needn't handle non-finite values.
Results may differ from the reference program's by a relative error of at most 0.0055.
Values may be sent and summed in bfloat16 or wider, within the bound.
A program may use at most 128 MiB of HBM per device.

```python
import math
import jax
import jax.numpy as jnp
from jax import lax

D = 1408
FF = 6144
TOK_DEV = 128
TOKENS = 32768
N_DP = 16
N_ROW = 8
N_COL = 2


def spiked(drawn, own_key, source, target, shards_of, factor):
    owner, partner = [(jnp.arange(drawn.shape[dim]) // (drawn.shape[dim] // shards_of)).reshape([-1 if axis == dim else 1 for axis in range(drawn.ndim)]) for dim in (source, target)]
    chosen = jax.random.permutation(own_key, shards_of)[partner]
    strong = (owner == chosen) | (owner == (partner + shards_of // 2) % shards_of)
    return jnp.where(strong, factor * drawn, drawn)


def block_levels(key, dims, split, smallest, largest):
    def one(axis_at, parts):
        steps = jax.random.uniform(jax.random.fold_in(jax.random.fold_in(key, 6), axis_at), (parts,), jnp.float32, smallest / len(split), largest / len(split))
        return jnp.repeat(jnp.exp(steps), dims[axis_at] // parts).reshape((-1,) + (1,) * (len(dims) - axis_at - 1))

    loudness = one(*split[0])
    for cut in split[1:]:
        loudness = loudness * one(*cut)
    return loudness


def noise(stream_key, shape, deviation, most, shards=(), kind=jnp.bfloat16):
    factor_of = block_levels(stream_key, shape, shards, -0.22, 0.18) if shards else 1.0
    result = jax.random.normal(stream_key, shape, jnp.float32) * deviation * factor_of
    return jnp.minimum(jnp.maximum(result, -most), most).astype(kind)


def noise_with(rng, dims, scale, reach, split, heavy, dtype=jnp.bfloat16):
    drawn = scale * jax.random.normal(rng, dims, jnp.float32)
    if split:
        drawn = drawn * block_levels(rng, dims, split, -0.22, 0.18)
    return jnp.clip(spiked(drawn, jax.random.fold_in(rng, 3), *heavy), -reach, reach).astype(dtype)


def setup_inputs(seed: int = 0) -> dict:
    arg_keys = jax.random.split(jax.random.key(seed), 9)
    return {
        "patches": noise(arg_keys[0], (TOKENS, D), 1.0, 6.0, ((0, 256),)),
        "norm_gain": jnp.clip(1.0 + 0.1 * jax.random.normal(arg_keys[1], (D,), jnp.float32), 0.5, 1.5),
        "norm_bias": noise(arg_keys[2], (D,), 0.5, 3.0, (), jnp.float32),
        "up_weight": noise(arg_keys[3], (D, FF), D ** -0.5, 0.15625, ((0, 2), (1, 8))),
        "up_bias": noise(arg_keys[4], (FF,), 0.5, 3.0, ((0, 8),), jnp.float32),
        "down_weight": noise(arg_keys[5], (FF, D), FF ** -0.5, 0.078125, ((0, 8), (1, 2))),
        "down_bias": noise(arg_keys[6], (D,), 0.5, 3.0, (), jnp.float32),
        "cotangent": noise_with(arg_keys[7], (TOKENS, D), 1.0, 24.0, ((0, 256),), (0, 1, 128, 5.5)),
    }


EPSILON = 1e-06
GELU_ROOT = 0.7978845608028654
GELU_CUBIC = 0.044715

def gelu_value(value):
    inner = jnp.tanh(GELU_ROOT * (value + GELU_CUBIC * value * value * value))
    return 0.5 * value * (1.0 + inner)

def gelu_slope(value):
    inner = jnp.tanh(GELU_ROOT * (value + GELU_CUBIC * value * value * value))
    return 0.5 * (1.0 + inner) + 0.5 * value * (1.0 - inner * inner) * GELU_ROOT * (1.0 + 3.0 * GELU_CUBIC * value * value)

def reference(patches, norm_gain, norm_bias, up_weight, up_bias, down_weight, down_bias, cotangent):
    replica_rows = TOK_DEV * N_ROW * N_COL
    patch_blocks = patches.reshape(N_DP, replica_rows, D)
    upstream_blocks = cotangent.reshape(N_DP, replica_rows, D)

    def one_block(carry, pieces):
        up_acc, down_acc, bias_acc, gain_acc, shift_acc = carry
        block, upstream = pieces
        wide = block.astype(jnp.float32)
        centred = wide - lax.optimization_barrier(jnp.mean(wide, axis=1, keepdims=True))
        inverse_spread = lax.rsqrt(lax.optimization_barrier(jnp.mean(centred * centred, axis=1, keepdims=True)) + EPSILON)
        standard = centred * inverse_spread
        normed = (standard * norm_gain + norm_bias).astype(jnp.bfloat16)
        preact = jnp.dot(normed, up_weight, preferred_element_type=jnp.float32) + up_bias
        activated = gelu_value(preact).astype(jnp.bfloat16)
        output = jnp.dot(activated, down_weight, preferred_element_type=jnp.float32) + down_bias + wide
        slope = (jnp.dot(upstream, down_weight.T, preferred_element_type=jnp.float32) * gelu_slope(preact)).astype(jnp.bfloat16)
        down_acc = down_acc + jnp.dot(activated.T, upstream, preferred_element_type=jnp.float32)
        up_acc = up_acc + jnp.dot(normed.T, slope, preferred_element_type=jnp.float32)
        bias_acc = bias_acc + lax.optimization_barrier(jnp.sum(slope.astype(jnp.float32), axis=0))
        normed_back = jnp.dot(slope, up_weight.T, preferred_element_type=jnp.float32)
        gain_acc = gain_acc + lax.optimization_barrier(jnp.sum(normed_back * standard, axis=0))
        shift_acc = shift_acc + lax.optimization_barrier(jnp.sum(normed_back, axis=0))
        scaled = normed_back * norm_gain
        back = inverse_spread * (scaled - lax.optimization_barrier(jnp.mean(scaled, axis=1, keepdims=True)) - standard * lax.optimization_barrier(jnp.mean(scaled * standard, axis=1, keepdims=True)))
        patch_grad = back + upstream.astype(jnp.float32)
        return ((up_acc, down_acc, bias_acc, gain_acc, shift_acc), (output, patch_grad))
    start = (jnp.zeros((D, FF), jnp.float32), jnp.zeros((FF, D), jnp.float32), jnp.zeros((FF,), jnp.float32), jnp.zeros((D,), jnp.float32), jnp.zeros((D,), jnp.float32))
    sums, results = lax.scan(one_block, start, (patch_blocks, upstream_blocks))
    scaling = 1.0 / math.sqrt(TOKENS)
    output = results[0].reshape(TOKENS, D)
    patch_grad = results[1].reshape(TOKENS, D)
    norm_grad = jnp.stack([sums[3], sums[4]]) * scaling
    return (output, patch_grad, sums[0] * scaling, sums[1] * scaling, sums[2] * scaling, norm_grad)
```

```python
import math

import jax
import jax.numpy as jnp
from jax import lax
from jax.experimental import pallas as pl
from jax.experimental.pallas import tpu as pltpu
from jax.sharding import Mesh
from jax.sharding import PartitionSpec as P

MESH = pl.DeviceIdType.MESH
ROW = ("row_0", "row_1")
DP_ROW_COL = ("dp_0", "dp_1", "row_0", "row_1", "col")

EPSILON = 1e-06
GELU_ROOT = 0.7978845608028654
GELU_CUBIC = 0.044715

D = 1408
HALF = 704
QUARTER = 352
HID = 768
TOK = 128
GROUP = 1024
CHUNK_ROWS, CHUNK_COLS, FIRST = 176, 384, 96
BF = jnp.bfloat16
F32 = jnp.float32


def aligned(value, tile):
    return pl.multiple_of(value, tile)


def step_kernel(
    patches, cotangent, gain, bias, up_bias, down_bias, up, down,
    out_proj, out_back, out_mine, out_other, out_small,
    normed, cot, up_all, down_all, bias_all, gelu_d, act, slope,
    part_out, part_back, core_out, core_back, far_out, far_back, near_out, near_back,
    grad_up, grad_down, far_up, far_down, own_up, near_a, near_b,
    zsum, z_far_a, z_far_b, z_near_a, z_near_b, mine, other,
    proj, back, bias_sum, small, small_core, small_y, small_x, small_z, small_total,
    send_sems, recv_sems, local_sems,
):
    z, c = lax.axis_index("dp_0"), lax.axis_index("dp_1")
    xl, y, xh = lax.axis_index("row_0"), lax.axis_index("row_1"), lax.axis_index("col")
    x = xh * 2 + xl
    owner = xl == c

    def x_dev(d, swap=False):
        there = lax.rem(x + d, 4)
        place = {"row_0": lax.rem(there, 2), "col": lax.div(there, 2)}
        return {**place, "dp_1": 1 - c} if swap else place

    def y_dev(d):
        return {"row_1": lax.rem(y + d, 4)}

    def z_dev(d):
        return {"dp_0": lax.rem(z + d, 8)}

    partner = {"dp_1": 1 - c}
    peers = [partner]
    peers += [x_dev(d) for d in (1, 2, 3)] + [x_dev(d, True) for d in (1, 3)]
    peers += [y_dev(d) for d in (1, 2, 3)] + [z_dev(d) for d in range(1, 8)]
    barrier = pltpu.get_barrier_semaphore()
    for peer in peers:
        pl.semaphore_signal(barrier, inc=1, device_id=peer, device_id_type=MESH)
    pl.semaphore_wait(barrier, len(peers))

    count = [0]

    class Link:
        def __init__(self, src, dst, device):
            self.k = count[0]
            count[0] += 1
            self.copy = pltpu.make_async_remote_copy(
                src_ref=src, dst_ref=dst, send_sem=send_sems.at[self.k], recv_sem=recv_sems.at[self.k],
                device_id=device, device_id_type=MESH,
            )

        def start(self):
            self.copy.start()
            return self

        def sent(self):
            self.copy.wait_send()

        def got(self, dst):
            pltpu.make_async_remote_copy(
                src_ref=dst, dst_ref=dst, send_sem=send_sems.at[self.k], recv_sem=recv_sems.at[self.k],
                device_id=partner, device_id_type=MESH,
            ).wait_recv()

    always, when_owner, when_relay = [], [], []

    h_me = xh
    h_next = lax.div(lax.rem(x + 1, 4), 2)
    h_prev = lax.div(lax.rem(x + 3, 4), 2)

    def part(ref, h, first):
        start = aligned(h * HALF + (0 if first else QUARTER), 16)
        return ref.at[pl.ds(start, QUARTER)]

    class Gather:
        def __init__(self, block, whole):
            self.block, self.whole = block, whole
            lo, hi = block.at[0:QUARTER], block.at[QUARTER:HALF]
            self.a1 = Link(lo, part(whole, h_me, True), x_dev(1))
            self.b2 = Link(hi, part(whole, h_me, False), x_dev(3))
            self.b1 = Link(hi, part(whole, h_me, False), x_dev(1))
            self.a2 = Link(lo, part(whole, h_me, True), x_dev(3))
            self.ra = Link(part(whole, h_prev, True), part(whole, h_prev, True), x_dev(1))
            self.rb = Link(part(whole, h_next, False), part(whole, h_next, False), x_dev(3))
            when_owner.extend([self.a1, self.b2, self.b1, self.a2])
            when_relay.extend([self.ra, self.rb])

        def begin(self):
            for link in (self.a1, self.b2, self.b1, self.a2):
                link.start()

        def relay(self):
            self.a1.got(part(self.whole, h_prev, True))
            self.ra.start()
            self.b2.got(part(self.whole, h_next, False))
            self.rb.start()

        def finish(self):
            @pl.when(owner)
            def _():
                self.ra.got(part(self.whole, 1 - h_me, True))
                self.rb.got(part(self.whole, 1 - h_me, False))

            @pl.when(jnp.logical_not(owner))
            def _():
                self.b1.got(part(self.whole, h_prev, False))
                self.a2.got(part(self.whole, h_next, True))

    ups, downs = Gather(up, up_all), Gather(down, down_all)
    bias_link = Link(up_bias, bias_all, x_dev(1))
    when_owner.append(bias_link)

    @pl.when(owner)
    def _():
        bias_link.start()
        ups.begin()
        downs.begin()
        bias_all[...] = up_bias[...]

    def slot(ref, dy, core, lo=0, rows=TOK):
        there = lax.rem(y + dy, 4)
        return ref.at[pl.ds(aligned((there * 2 + core) * TOK + lo, 16), rows)]

    class Tokens:
        def __init__(self, own, whole):
            self.whole = whole
            self.next = Link(own, slot(whole, 0, c), y_dev(1)).start()
            self.prev = Link(own, slot(whole, 0, c), y_dev(3)).start()
            self.over = Link(own, slot(whole, 0, c), partner).start()
            always.extend([self.next, self.prev, self.over])

        def relay(self):
            whole = self.whole
            self.next.got(slot(whole, 3, c))
            self.far_a = Link(slot(whole, 3, c, 0, 64), slot(whole, 3, c, 0, 64), y_dev(1)).start()
            self.over_a = Link(slot(whole, 3, c), slot(whole, 3, c), partner).start()
            self.prev.got(slot(whole, 1, c))
            self.far_b = Link(slot(whole, 1, c, 64, 64), slot(whole, 1, c, 64, 64), y_dev(3)).start()
            self.over_b = Link(slot(whole, 1, c), slot(whole, 1, c), partner).start()
            always.extend([self.far_a, self.over_a, self.far_b, self.over_b])

        def finish(self):
            whole = self.whole
            self.far_a.got(slot(whole, 2, c, 0, 64))
            self.far_b.got(slot(whole, 2, c, 64, 64))
            self.over_far = Link(slot(whole, 2, c), slot(whole, 2, c), partner).start()
            always.append(self.over_far)
            self.over.got(slot(whole, 0, 1 - c))
            self.over_a.got(slot(whole, 3, 1 - c))
            self.over_b.got(slot(whole, 1, 1 - c))
            self.over_far.got(slot(whole, 2, 1 - c))

    def spread():
        wide = patches[...].astype(F32)
        centred = wide - jnp.mean(wide, axis=1, keepdims=True)
        inverse = lax.rsqrt(jnp.mean(centred * centred, axis=1, keepdims=True) + EPSILON)
        return centred * inverse, inverse

    own_rows = pl.ds(aligned((y * 2 + c) * TOK, TOK), TOK)
    normed[own_rows] = (spread()[0] * gain[...] + bias[...]).astype(BF)
    tok_n = Tokens(normed.at[own_rows], normed)
    tok_c = Tokens(cotangent, cot)
    cot[own_rows] = cotangent[...]

    @pl.when(owner)
    def _():
        rows = pl.ds(aligned(h_me * HALF, 16), HALF)
        up_all[rows] = up[...]
        down_all[rows] = down[...]

    tok_n.relay()

    @pl.when(jnp.logical_not(owner))
    def _():
        bias_link.got(bias_all)
        ups.relay()

    tok_n.finish()
    ups.finish()

    @pl.loop(0, GROUP // 256)
    def _(i):
        rows = pl.ds(aligned(i * 256, 256), 256)
        v = jnp.dot(normed[rows], up_all[...], preferred_element_type=F32) + bias_all[...]
        inner = jnp.tanh(GELU_ROOT * (v + GELU_CUBIC * v * v * v))
        act[rows] = (0.5 * v * (1.0 + inner)).astype(BF)
        gelu_d[rows] = 0.5 * (1.0 + inner) + 0.5 * v * (1.0 - inner * inner) * GELU_ROOT * (
            1.0 + 3.0 * GELU_CUBIC * v * v
        )

    tok_c.relay()

    @pl.when(jnp.logical_not(owner))
    def _():
        downs.relay()

    tok_c.finish()

    def outer(left, right, result):
        for lo, hi in ((0, 512), (512, 1024), (1024, D)):
            result[lo:hi] = lax.dot_general(
                left[:, lo:hi], right[...], (((0,), (0,)), ((), ())), preferred_element_type=F32
            ).astype(BF)

    class Reduce:
        def __init__(self, grad, far, swap):
            self.grad, self.far = grad, far
            h_far = 1 - h_me
            self.s0 = Link(part(grad, h_far, True), far.at[0], x_dev(1))
            self.s1 = Link(part(grad, h_far, False), far.at[1], x_dev(3))
            when_owner.extend([self.s0, self.s1])
            lo, hi = pl.ds(0, QUARTER), pl.ds(QUARTER, QUARTER)
            self.s2 = Link(part(grad, h_next, False), near_a.at[hi], x_dev(1, swap))
            self.s4 = Link(part(grad, h_prev, True), near_b.at[lo], x_dev(3, swap))
            self.s3 = Link(part(grad, h_next, True), near_a.at[lo], x_dev(1, swap))
            self.s5 = Link(part(grad, h_prev, False), near_b.at[hi], x_dev(3, swap))
            when_relay.extend([self.s2, self.s4, self.s3, self.s5])

        def begin(self):
            @pl.when(owner)
            def _():
                self.s0.start()
                self.s1.start()

            @pl.when(jnp.logical_not(owner))
            def _():
                self.s2.start()
                self.s4.start()

        def middle(self):
            grad, far = self.grad, self.far

            @pl.when(jnp.logical_not(owner))
            def _():
                for link, other_link, h, first, k in ((self.s0, self.s3, h_next, True, 0), (self.s1, self.s5, h_prev, False, 1)):
                    link.got(far.at[k])
                    rows = pl.ds(aligned(h * HALF + (0 if first else QUARTER), 16), QUARTER)
                    grad[rows] = (grad[rows].astype(F32) + far[k].astype(F32)).astype(BF)
                    other_link.start()

        def finish(self):
            lo, hi = pl.ds(0, QUARTER), pl.ds(QUARTER, QUARTER)
            self.s2.got(near_a.at[hi])
            self.s4.got(near_b.at[lo])
            self.s3.got(near_a.at[lo])
            self.s5.got(near_b.at[hi])

    red_down = Reduce(grad_down, far_down, False)
    red_up = Reduce(grad_up, far_up, True)
    own_rows_w = pl.ds(aligned(h_me * HALF, 16), HALF)
    own_link = Link(grad_up.at[own_rows_w], own_up, partner)
    when_owner.append(own_link)

    outer(cot, act, grad_down)
    red_down.begin()
    downs.finish()

    bias_sum[...] = jnp.zeros_like(bias_sum)

    @pl.loop(0, GROUP // 256)
    def _(i):
        rows = pl.ds(aligned(i * 256, 256), 256)
        s = jnp.dot(cot[rows], down_all[...], preferred_element_type=F32) * gelu_d[rows]
        s = s.astype(BF)
        slope[rows] = s
        bias_sum[...] += jnp.sum(s.astype(F32), axis=0, keepdims=True)

    outer(normed, slope, grad_up)
    red_up.begin()

    @pl.when(owner)
    def _():
        own_link.start()

    red_down.middle()

    def across(left, right, result):
        @pl.loop(0, GROUP // 256)
        def _(i):
            rows = pl.ds(aligned(i * 256, 256), 256)
            result[rows] = lax.dot_general(
                left[rows], right[...], (((1,), (1,)), ((), ())), preferred_element_type=F32
            ).astype(BF)

    class Scatter:
        def __init__(self, partial, core, far, near):
            self.partial, self.core, self.far, self.near = partial, core, far, near
            self.over = []
            for dy in (2, 1, 3, 0):
                there = lax.rem(y + dy, 4)
                self.over.append((dy, Link(slot(partial, dy, 1 - c), core.at[there], partner).start()))
            always.extend(link for _, link in self.over)

        def combine(self):
            partial, core = self.partial, self.core
            for dy, link in self.over:
                there = lax.rem(y + dy, 4)
                link.got(core.at[there])
                if dy == 0:
                    continue
                rows = pl.ds(aligned((there * 2 + c) * TOK, TOK), TOK)
                partial[rows] = (partial[rows].astype(F32) + core[there].astype(F32)).astype(BF)
                if dy == 2:
                    self.t0 = Link(slot(partial, 2, c, 0, 64), self.far.at[0], y_dev(1)).start()
                    self.t1 = Link(slot(partial, 2, c, 64, 64), self.far.at[1], y_dev(3)).start()
                elif dy == 1:
                    self.t2 = Link(slot(partial, 1, c, 64, 64), self.near.at[0, pl.ds(64, 64)], y_dev(1)).start()
                else:
                    self.t3 = Link(slot(partial, 3, c, 0, 64), self.near.at[1, pl.ds(0, 64)], y_dev(3)).start()
            always.extend([self.t0, self.t1, self.t2, self.t3])

        def middle(self):
            partial, far = self.partial, self.far
            for dy, lo, k, link in ((1, 0, 0, self.t0), (3, 64, 1, self.t1)):
                link.got(far.at[k])
                there = lax.rem(y + dy, 4)
                rows = pl.ds(aligned((there * 2 + c) * TOK + lo, 16), 64)
                partial[rows] = (partial[rows].astype(F32) + far[k].astype(F32)).astype(BF)
                onward = Link(slot(partial, dy, c, lo, 64), self.near.at[k, pl.ds(lo, 64)], y_dev(dy)).start()
                always.append(onward)
                if k == 0:
                    self.t4 = onward
                else:
                    self.t5 = onward

        def finish(self):
            near = self.near
            self.t2.got(near.at[0, pl.ds(64, 64)])
            self.t3.got(near.at[1, pl.ds(0, 64)])
            self.t4.got(near.at[0, pl.ds(0, 64)])
            self.t5.got(near.at[1, pl.ds(64, 64)])
            own = self.partial[own_rows].astype(F32) + self.core[y].astype(F32)
            return own + near[0].astype(F32) + near[1].astype(F32)

    across(slope, up_all, part_back)
    sc_back = Scatter(part_back, core_back, far_back, near_back)
    across(act, down_all, part_out)
    sc_out = Scatter(part_out, core_out, far_out, near_out)
    sc_back.combine()
    sc_out.combine()
    red_up.middle()
    sc_back.middle()
    sc_out.middle()

    back[...] = sc_back.finish()
    standard, inverse = spread()
    nb = back[...]
    rows_small = (
        (0, D // 128, jnp.sum(nb * standard, axis=0, keepdims=True)),
        (D // 128, D // 128, jnp.sum(nb, axis=0, keepdims=True)),
        (2 * (D // 128), HID // 128, bias_sum[...]),
    )
    small[...] = jnp.zeros_like(small)
    for first, length, row in rows_small:
        for i in range(length):
            small[first + i : first + i + 1, :] = row[:, 128 * i : 128 * (i + 1)]
    n_norm = 2 * (D // 128)
    small_over = Link(small, small_core, partner).start()
    always.append(small_over)
    scaled = nb * gain[...]
    back[...] = inverse * (
        scaled
        - jnp.mean(scaled, axis=1, keepdims=True)
        - standard * jnp.mean(scaled * standard, axis=1, keepdims=True)
    )
    put_back = pltpu.make_async_copy(back, out_back, local_sems.at[0])
    put_back.start()

    def load_own(source):
        for k in range(8):
            r = slice((k % 4) * CHUNK_ROWS, (k % 4 + 1) * CHUNK_ROWS)
            l = slice((k // 4) * CHUNK_COLS, (k // 4 + 1) * CHUNK_COLS)
            zsum[k] = (
                source(k).astype(F32) + near_a[r, l].astype(F32) + near_b[r, l].astype(F32)
            ).astype(BF)

    @pl.when(owner)
    def _():
        red_down.finish()

        def source(k):
            rows = pl.ds(aligned(h_me * HALF + (k % 4) * CHUNK_ROWS, 16), CHUNK_ROWS)
            return grad_down[rows, (k // 4) * CHUNK_COLS : (k // 4 + 1) * CHUNK_COLS]

        load_own(source)

    @pl.when(jnp.logical_not(owner))
    def _():
        own_link.got(own_up)
        red_up.finish()

        def source(k):
            return own_up[
                (k % 4) * CHUNK_ROWS : (k % 4 + 1) * CHUNK_ROWS, (k // 4) * CHUNK_COLS : (k // 4 + 1) * CHUNK_COLS
            ]

        load_own(source)

    def at_z(d):
        return lax.rem(z + d, 8)

    head, tail = pl.ds(0, FIRST), pl.ds(FIRST, CHUNK_ROWS - FIRST)
    f0 = Link(zsum.at[at_z(4), head], z_far_a, z_dev(1)).start()
    b0 = Link(zsum.at[at_z(4), tail], z_far_b, z_dev(7)).start()
    always.extend([f0, b0])

    def add_rows(k, rows, incoming):
        zsum[k, rows] = (zsum[k, rows].astype(F32) + incoming.astype(F32)).astype(BF)

    small_over.got(small_core)
    keep = lax.broadcasted_iota(jnp.int32, small.shape, 0) < n_norm
    small_y[y] = small[...] + jnp.where(keep, small_core[...], 0.0)
    y_links = [Link(small_y.at[y], small_y.at[y], y_dev(d)).start() for d in (1, 2, 3)]
    always.extend(y_links)

    f0.got(z_far_a)
    add_rows(at_z(3), head, z_far_a[...])
    f1 = Link(zsum.at[at_z(3)], z_near_a.at[0], z_dev(1)).start()
    b0.got(z_far_b)
    add_rows(at_z(5), tail, z_far_b[...])
    b1 = Link(zsum.at[at_z(5)], z_near_b.at[0], z_dev(7)).start()
    always.extend([f1, b1])

    for d, link in zip((1, 2, 3), y_links):
        link.got(small_y.at[lax.rem(y + 4 - d, 4)])
    ysum = small_y[0] + small_y[1] + small_y[2] + small_y[3]
    small_x[x] = jnp.where(keep, ysum, small[...])
    x_links = [Link(small_x.at[x], small_x.at[x], x_dev(d)).start() for d in (1, 2, 3)]
    always.extend(x_links)

    everything = pl.ds(0, CHUNK_ROWS)
    f1.got(z_near_a.at[0])
    add_rows(at_z(2), everything, z_near_a[0])
    f2 = Link(zsum.at[at_z(2)], z_near_a.at[1], z_dev(1)).start()
    b1.got(z_near_b.at[0])
    add_rows(at_z(6), everything, z_near_b[0])
    b2 = Link(zsum.at[at_z(6)], z_near_b.at[1], z_dev(7)).start()
    always.extend([f2, b2])

    for d, link in zip((1, 2, 3), x_links):
        link.got(small_x.at[lax.rem(x + 4 - d, 4)])
    small_z[z] = small_x[0] + small_x[1] + small_x[2] + small_x[3]
    z_links = [Link(small_z.at[z], small_z.at[z], z_dev(d)).start() for d in range(1, 8)]
    always.extend(z_links)

    f2.got(z_near_a.at[1])
    add_rows(at_z(1), everything, z_near_a[1])
    f3 = Link(zsum.at[at_z(1)], z_near_a.at[2], z_dev(1)).start()
    b2.got(z_near_b.at[1])
    add_rows(at_z(7), everything, z_near_b[1])
    b3 = Link(zsum.at[at_z(7)], z_near_b.at[2], z_dev(7)).start()
    always.extend([f3, b3])

    for d, link in zip(range(1, 8), z_links):
        link.got(small_z.at[at_z(8 - d)])
    total = small_z[0]
    for k in range(1, 8):
        total = total + small_z[k]
    small_total[0] = total
    last_over = Link(small_total.at[0], small_total.at[1], partner).start()
    always.append(last_over)

    f3.got(z_near_a.at[2])
    b3.got(z_near_b.at[2])
    mine[z] = (zsum[z].astype(F32) + z_near_a[2].astype(F32) + z_near_b[2].astype(F32)).astype(BF)

    def forward(k, device):
        link = Link(mine.at[k], mine.at[k], device).start()
        always.append(link)
        return link

    overs = []

    def hand_over(k):
        link = Link(mine.at[k], other.at[k], partner).start()
        always.append(link)
        overs.append((link, k))

    ga = forward(z, z_dev(1))
    gb = forward(z, z_dev(7))
    hand_over(z)
    for d in (1, 2):
        ga.got(mine.at[at_z(8 - d)])
        ga = forward(at_z(8 - d), z_dev(1))
        hand_over(at_z(8 - d))
        gb.got(mine.at[at_z(d)])
        gb = forward(at_z(d), z_dev(7))
        hand_over(at_z(d))
    ga.got(mine.at[at_z(5)])
    ha = Link(mine.at[at_z(5), head], mine.at[at_z(5), head], z_dev(1)).start()
    hand_over(at_z(5))
    gb.got(mine.at[at_z(3)])
    hb = Link(mine.at[at_z(3), tail], mine.at[at_z(3), tail], z_dev(7)).start()
    hand_over(at_z(3))
    always.extend([ha, hb])

    proj[...] = sc_out.finish() + down_bias[...]
    put_proj = pltpu.make_async_copy(proj, out_proj, local_sems.at[1])
    put_proj.start()

    ha.got(mine.at[at_z(4), head])
    hb.got(mine.at[at_z(4), tail])
    hand_over(at_z(4))
    put_mine = pltpu.make_async_copy(mine, out_mine, local_sems.at[2])
    put_mine.start()
    for link, k in overs:
        link.got(other.at[k])
    put_other = pltpu.make_async_copy(other, out_other, local_sems.at[3])
    put_other.start()
    last_over.got(small_total.at[1])
    put_small = pltpu.make_async_copy(small_total, out_small, local_sems.at[4])
    put_small.start()

    for link in always:
        link.sent()

    @pl.when(owner)
    def _():
        for link in when_owner:
            link.sent()

    @pl.when(jnp.logical_not(owner))
    def _():
        for link in when_relay:
            link.sent()

    for put in (put_back, put_proj, put_mine, put_other, put_small):
        put.wait()
    assert count[0] <= N_LINKS


N_LINKS = 128


def on_device(patches, norm_gain, norm_bias, up_weight, up_bias, down_weight, down_bias, cotangent):
    scaling = 1.0 / math.sqrt(TOK * 256)
    vmem = pl.BlockSpec(memory_space=pltpu.VMEM)
    hbm = pl.BlockSpec(memory_space=pl.ANY)

    def V(*shape, dtype=BF):
        return pltpu.VMEM(shape, dtype)

    proj, back, mine, other, small = pl.pallas_call(
        step_kernel,
        out_shape=(
            jax.ShapeDtypeStruct((TOK, D), F32),
            jax.ShapeDtypeStruct((TOK, D), F32),
            jax.ShapeDtypeStruct((8, CHUNK_ROWS, CHUNK_COLS), BF),
            jax.ShapeDtypeStruct((8, CHUNK_ROWS, CHUNK_COLS), BF),
            jax.ShapeDtypeStruct((2, 32, 128), F32),
        ),
        in_specs=[vmem] * 8,
        out_specs=[hbm] * 5,
        scratch_shapes=[
            V(GROUP, D), V(GROUP, D), V(D, HID), V(D, HID), V(1, HID, dtype=F32),
            V(GROUP, HID, dtype=F32), V(GROUP, HID), V(GROUP, HID),
            V(GROUP, D), V(GROUP, D), V(4, TOK, D), V(4, TOK, D),
            V(2, 64, D), V(2, 64, D), V(2, TOK, D), V(2, TOK, D),
            V(D, HID), V(D, HID), V(2, QUARTER, HID), V(2, QUARTER, HID), V(HALF, HID),
            V(HALF, HID), V(HALF, HID),
            V(8, CHUNK_ROWS, CHUNK_COLS), V(FIRST, CHUNK_COLS), V(CHUNK_ROWS - FIRST, CHUNK_COLS),
            V(3, CHUNK_ROWS, CHUNK_COLS), V(3, CHUNK_ROWS, CHUNK_COLS),
            V(8, CHUNK_ROWS, CHUNK_COLS), V(8, CHUNK_ROWS, CHUNK_COLS),
            V(TOK, D, dtype=F32), V(TOK, D, dtype=F32), V(1, HID, dtype=F32),
            V(32, 128, dtype=F32), V(32, 128, dtype=F32), V(4, 32, 128, dtype=F32),
            V(4, 32, 128, dtype=F32), V(8, 32, 128, dtype=F32), V(2, 32, 128, dtype=F32),
            pltpu.SemaphoreType.DMA((N_LINKS,)),
            pltpu.SemaphoreType.DMA((N_LINKS,)),
            pltpu.SemaphoreType.DMA((5,)),
        ],
        compiler_params=pltpu.CompilerParams(
            collective_id=0, has_side_effects=True, vmem_limit_bytes=63 * 1024 * 1024
        ),
    )(
        patches, cotangent, norm_gain[None], norm_bias[None], up_bias[None], down_bias[None],
        up_weight, down_weight.T,
    )

    owner = lax.axis_index("row_0") == lax.axis_index("dp_1")

    def whole(chunks):
        left, right = chunks.reshape(2, HALF, CHUNK_COLS)
        return jnp.concatenate([left, right], axis=1).astype(F32) * scaling

    up_grad = whole(jnp.where(owner, other, mine))
    down_grad = whole(jnp.where(owner, mine, other)).T
    small = small * scaling
    n = D // 128
    norm_grad = small[0, : 2 * n].reshape(2, D)
    bias_grad = jnp.where(owner, small[0], small[1])[2 * n : 2 * n + HID // 128].reshape(HID)
    output = proj + patches.astype(F32)
    patch_grad = back + cotangent.astype(F32)
    return output, patch_grad, up_grad, down_grad, bias_grad, norm_grad


def solution(mesh):
    split = Mesh(
        mesh.devices.reshape(8, 2, 2, 4, mesh.shape["col"]),
        ("dp_0", "dp_1", "row_0", "row_1", "col"),
    )
    return jax.shard_map(
        on_device,
        mesh=split,
        in_specs=(
            P(DP_ROW_COL, None), P(), P(), P("col", ROW), P(ROW), P(ROW, "col"), P(), P(DP_ROW_COL, None),
        ),
        out_specs=(
            P(DP_ROW_COL, None), P(DP_ROW_COL, None), P("col", ROW), P(ROW, "col"), P(ROW), P(),
        ),
        check_vma=False,
    )
```

```python
import math

import jax
import jax.numpy as jnp
from jax import lax
from jax.experimental import pallas as pl
from jax.experimental.pallas import tpu as pltpu
from jax.sharding import Mesh
from jax.sharding import PartitionSpec as P

MESH = pl.DeviceIdType.MESH
ROW = ("row_0", "row_1")
DP_ROW_COL = ("dp_0", "dp_1", "row_0", "row_1", "col")

EPSILON = 1e-06
GELU_ROOT = 0.7978845608028654
GELU_CUBIC = 0.044715

D = 1408
HALF = 704
QUARTER = 352
HID = 768
TOK = 128
GROUP = 1024
CHUNK_ROWS, CHUNK_COLS = 176, 384
UNITS = (pl.ds(0, 96), pl.ds(96, 80))
BF = jnp.bfloat16
F32 = jnp.float32


def aligned(value, tile):
    return pl.multiple_of(value, tile)


def step_kernel(
    patches_in, cotangent_in, gain, bias, up_bias, down_bias, up, down,
    out_proj, out_back, out_mine, out_other, out_small,
    patches, normed, cot, up_all, down_all, bias_all, gelu_d, act, slope,
    part_out, part_back, core_out, core_back, far_out, far_back, near_out, near_back,
    grad_up, grad_down, far_up, far_down, own_up, near_a, near_b,
    zsum, z_near_a, z_near_b, mine, other,
    proj, back, bias_sum, small, small_core, small_y, small_x, small_z, small_total,
    send_sems, recv_sems, local_sems,
):
    z, c = lax.axis_index("dp_0"), lax.axis_index("dp_1")
    xl, y, xh = lax.axis_index("row_0"), lax.axis_index("row_1"), lax.axis_index("col")
    x = xh * 2 + xl
    owner = xl == c

    def x_dev(d, swap=False):
        there = lax.rem(x + d, 4)
        place = {"row_0": lax.rem(there, 2), "col": lax.div(there, 2)}
        return {**place, "dp_1": 1 - c} if swap else place

    def y_dev(d):
        return {"row_1": lax.rem(y + d, 4)}

    def z_dev(d):
        return {"dp_0": lax.rem(z + d, 8)}

    partner = {"dp_1": 1 - c}
    peers = [partner]
    peers += [x_dev(d) for d in (1, 2, 3)] + [x_dev(d, True) for d in (1, 3)]
    peers += [y_dev(d) for d in (1, 2, 3)] + [z_dev(d) for d in range(1, 8)]
    own_rows = pl.ds(aligned((y * 2 + c) * TOK, TOK), TOK)
    own_block = pl.ds(aligned(xh * HALF, 16), HALF)
    load_patches = pltpu.make_async_copy(patches_in, patches, local_sems.at[5])
    load_cot = pltpu.make_async_copy(cotangent_in, cot.at[own_rows], local_sems.at[6])
    load_up = pltpu.make_async_copy(up, up_all.at[own_block], local_sems.at[7])
    load_down = pltpu.make_async_copy(down, down_all.at[own_block], local_sems.at[8])
    load_patches.start()
    load_cot.start()

    @pl.when(owner)
    def _():
        load_up.start()
        load_down.start()

    barrier = pltpu.get_barrier_semaphore()
    for peer in peers:
        pl.semaphore_signal(barrier, inc=1, device_id=peer, device_id_type=MESH)
    pl.semaphore_wait(barrier, len(peers))

    count = [0]

    class Link:
        def __init__(self, src, dst, device):
            self.k = count[0]
            count[0] += 1
            self.copy = pltpu.make_async_remote_copy(
                src_ref=src, dst_ref=dst, send_sem=send_sems.at[self.k], recv_sem=recv_sems.at[self.k],
                device_id=device, device_id_type=MESH,
            )

        def start(self):
            self.copy.start()
            return self

        def sent(self):
            self.copy.wait_send()

        def got(self, dst):
            pltpu.make_async_remote_copy(
                src_ref=dst, dst_ref=dst, send_sem=send_sems.at[self.k], recv_sem=recv_sems.at[self.k],
                device_id=partner, device_id_type=MESH,
            ).wait_recv()

    always, when_owner, when_relay = [], [], []

    h_me = xh
    h_next = lax.div(lax.rem(x + 1, 4), 2)
    h_prev = lax.div(lax.rem(x + 3, 4), 2)

    lanes_x = pl.ds(aligned(lax.rem(z, 2) * CHUNK_COLS, 128), CHUNK_COLS)
    lanes_z = pl.ds(aligned((1 - lax.rem(z, 2)) * CHUNK_COLS, 128), CHUNK_COLS)

    def part(ref, h, first, lanes):
        start = aligned(h * HALF + (0 if first else QUARTER), 16)
        return ref.at[pl.ds(start, QUARTER), lanes]

    class Gather:
        def __init__(self, whole):
            def link(h, first, device):
                return Link(part(whole, h, first, lanes_x), part(whole, h, first, lanes_x), device)

            self.whole = whole
            self.a1, self.b2 = link(h_me, True, x_dev(1)), link(h_me, False, x_dev(3))
            self.b1, self.a2 = link(h_me, False, x_dev(1)), link(h_me, True, x_dev(3))
            self.ra, self.rb = link(h_prev, True, x_dev(1)), link(h_next, False, x_dev(3))
            self.oa, self.ob = link(1 - h_me, True, z_dev(1)), link(1 - h_me, False, z_dev(7))
            self.pa, self.nb = link(h_prev, True, z_dev(1)), link(h_next, False, z_dev(7))
            self.pb, self.na = link(h_prev, False, z_dev(7)), link(h_next, True, z_dev(1))
            when_owner.extend([self.a1, self.b2, self.b1, self.a2, self.oa, self.ob])
            when_relay.extend([self.ra, self.rb, self.pa, self.nb, self.pb, self.na])

        def here(self, h, first):
            return part(self.whole, h, first, lanes_x)

        def there(self, h, first):
            return part(self.whole, h, first, lanes_z)

        def begin(self):
            for link in (self.a1, self.b2, self.b1, self.a2):
                link.start()

        def relay(self):
            self.a1.got(self.here(h_prev, True))
            self.ra.start()
            self.pa.start()
            self.b2.got(self.here(h_next, False))
            self.rb.start()
            self.nb.start()

        def relay_last(self):
            self.b1.got(self.here(h_prev, False))
            self.pb.start()
            self.a2.got(self.here(h_next, True))
            self.na.start()

        def pass_on(self):
            self.ra.got(self.here(1 - h_me, True))
            self.oa.start()
            self.rb.got(self.here(1 - h_me, False))
            self.ob.start()

        def finish(self):
            @pl.when(owner)
            def _():
                self.oa.got(self.there(1 - h_me, True))
                self.ob.got(self.there(1 - h_me, False))

            @pl.when(jnp.logical_not(owner))
            def _():
                self.pa.got(self.there(h_prev, True))
                self.nb.got(self.there(h_next, False))
                self.pb.got(self.there(h_prev, False))
                self.na.got(self.there(h_next, True))

    ups, downs = Gather(up_all), Gather(down_all)
    bias_link = Link(up_bias, bias_all, x_dev(1))
    when_owner.append(bias_link)

    @pl.when(owner)
    def _():
        load_up.wait()
        ups.begin()
        bias_link.start()
        load_down.wait()
        downs.begin()
        bias_all[...] = up_bias[...]

    def slot(ref, dy, core, lo=0, rows=TOK):
        there = lax.rem(y + dy, 4)
        return ref.at[pl.ds(aligned((there * 2 + core) * TOK + lo, 16), rows)]

    class Tokens:
        def __init__(self, own, whole):
            self.whole = whole
            self.next = Link(own, slot(whole, 0, c), y_dev(1)).start()
            self.prev = Link(own, slot(whole, 0, c), y_dev(3)).start()
            self.over = Link(own, slot(whole, 0, c), partner).start()
            always.extend([self.next, self.prev, self.over])

        def relay(self):
            whole = self.whole
            self.next.got(slot(whole, 3, c))
            self.far_a = Link(slot(whole, 3, c, 0, 64), slot(whole, 3, c, 0, 64), y_dev(1)).start()
            self.over_a = Link(slot(whole, 3, c), slot(whole, 3, c), partner).start()
            self.prev.got(slot(whole, 1, c))
            self.far_b = Link(slot(whole, 1, c, 64, 64), slot(whole, 1, c, 64, 64), y_dev(3)).start()
            self.over_b = Link(slot(whole, 1, c), slot(whole, 1, c), partner).start()
            always.extend([self.far_a, self.over_a, self.far_b, self.over_b])

        def finish(self):
            whole = self.whole
            self.far_a.got(slot(whole, 2, c, 0, 64))
            self.far_b.got(slot(whole, 2, c, 64, 64))
            self.over_far = Link(slot(whole, 2, c), slot(whole, 2, c), partner).start()
            always.append(self.over_far)
            self.over.got(slot(whole, 0, 1 - c))
            self.over_a.got(slot(whole, 3, 1 - c))
            self.over_b.got(slot(whole, 1, 1 - c))
            self.over_far.got(slot(whole, 2, 1 - c))

    def spread():
        wide = patches[...].astype(F32)
        centred = wide - jnp.mean(wide, axis=1, keepdims=True)
        inverse = lax.rsqrt(jnp.mean(centred * centred, axis=1, keepdims=True) + EPSILON)
        return centred * inverse, inverse

    load_cot.wait()
    load_patches.wait()
    normed[own_rows] = (spread()[0] * gain[...][None] + bias[...][None]).astype(BF)
    tok_n = Tokens(normed.at[own_rows], normed)
    tok_c = Tokens(cot.at[own_rows], cot)

    @pl.when(jnp.logical_not(owner))
    def _():
        ups.relay()

    tok_n.relay()

    @pl.when(owner)
    def _():
        ups.pass_on()

    @pl.when(jnp.logical_not(owner))
    def _():
        bias_link.got(bias_all)
        ups.relay_last()
        downs.relay()

    tok_c.relay()

    @pl.when(owner)
    def _():
        downs.pass_on()

    @pl.when(jnp.logical_not(owner))
    def _():
        downs.relay_last()

    tok_n.finish()
    ups.finish()

    @pl.loop(0, GROUP // 256)
    def _(i):
        rows = pl.ds(aligned(i * 256, 256), 256)
        v = jnp.dot(normed[rows], up_all[...], preferred_element_type=F32) + bias_all[...][None]
        inner = jnp.tanh(GELU_ROOT * (v + GELU_CUBIC * v * v * v))
        act[rows] = (0.5 * v * (1.0 + inner)).astype(BF)
        gelu_d[rows] = 0.5 * (1.0 + inner) + 0.5 * v * (1.0 - inner * inner) * GELU_ROOT * (
            1.0 + 3.0 * GELU_CUBIC * v * v
        )

    tok_c.finish()

    def outer(left, right, result):
        for lo, hi in ((0, 512), (512, 1024), (1024, D)):
            block = lax.dot_general(
                left[:, lo:hi], right[...], (((0,), (0,)), ((), ())), preferred_element_type=F32
            ).astype(BF)
            while lo < hi:
                j, r = divmod(lo, CHUNK_ROWS)
                rows = min(CHUNK_ROWS - r, hi - lo)
                result[j, r : r + rows] = block[:rows]
                block, lo = block[rows:], lo + rows

    class Reduce:
        def __init__(self, grad, far, swap):
            self.grad, self.far, self.links = grad, far, []
            lo, hi = pl.ds(0, 2), pl.ds(2, 2)
            for rows in UNITS:
                s0 = Link(self.of(1 - h_me, True, rows), far.at[lo, rows], x_dev(1))
                s1 = Link(self.of(1 - h_me, False, rows), far.at[hi, rows], x_dev(3))
                s2 = Link(self.of(h_next, False, rows), near_a.at[hi, rows], x_dev(1, swap))
                s4 = Link(self.of(h_prev, True, rows), near_b.at[lo, rows], x_dev(3, swap))
                s3 = Link(self.of(h_next, True, rows), near_a.at[lo, rows], x_dev(1, swap))
                s5 = Link(self.of(h_prev, False, rows), near_b.at[hi, rows], x_dev(3, swap))
                when_owner.extend([s0, s1])
                when_relay.extend([s2, s4, s3, s5])
                self.links.append((s0, s1, s2, s3, s4, s5))

        def of(self, h, first, rows):
            return self.grad.at[pl.ds(h * 4 + (0 if first else 2), 2), rows]

        def send_far(self, u):
            s0, s1, _, _, _, _ = self.links[u]
            s0.start()
            s1.start()

        def send_near(self, u):
            _, _, s2, _, s4, _ = self.links[u]
            s2.start()
            s4.start()

        def middle(self, u):
            grad, far, rows = self.grad, self.far, UNITS[u]
            s0, s1, _, s3, _, s5 = self.links[u]
            for link, onward, h, first, k in ((s0, s3, h_next, True, 0), (s1, s5, h_prev, False, 2)):
                link.got(far.at[pl.ds(k, 2), rows])
                for j in (0, 1):
                    at = h * 4 + (0 if first else 2) + j
                    grad[at, rows] = (grad[at, rows].astype(F32) + far[k + j, rows].astype(F32)).astype(BF)
                onward.start()

        def finish(self, u):
            _, _, s2, s3, s4, s5 = self.links[u]
            lo, hi, rows = pl.ds(0, 2), pl.ds(2, 2), UNITS[u]
            s2.got(near_a.at[hi, rows])
            s4.got(near_b.at[lo, rows])
            s3.got(near_a.at[lo, rows])
            s5.got(near_b.at[hi, rows])

    red_down = Reduce(grad_down, far_down, False)
    red_up = Reduce(grad_up, far_up, True)
    own_link = Link(grad_up.at[pl.ds(h_me * 4, 4)], own_up, partner)
    when_owner.append(own_link)
    not_owner = jnp.logical_not(owner)

    outer(cot, act, grad_down)

    @pl.when(owner)
    def _():
        red_down.send_far(0)
        red_down.send_far(1)

    @pl.when(not_owner)
    def _():
        red_down.send_near(0)
        red_down.send_near(1)

    downs.finish()

    bias_sum[...] = jnp.zeros_like(bias_sum)

    @pl.loop(0, GROUP // 256)
    def _(i):
        rows = pl.ds(aligned(i * 256, 256), 256)
        s = jnp.dot(cot[rows], down_all[...], preferred_element_type=F32) * gelu_d[rows]
        s = s.astype(BF)
        slope[rows] = s
        bias_sum[...] += jnp.sum(s.astype(F32), axis=0, keepdims=True)

    outer(normed, slope, grad_up)

    @pl.when(owner)
    def _():
        own_link.start()
        red_up.send_far(0)
        red_up.send_far(1)

    @pl.when(not_owner)
    def _():
        red_down.middle(0)
        red_up.send_near(0)

    def across(left, right, result):
        @pl.loop(0, GROUP // 256)
        def _(i):
            rows = pl.ds(aligned(i * 256, 256), 256)
            result[rows] = lax.dot_general(
                left[rows], right[...], (((1,), (1,)), ((), ())), preferred_element_type=F32
            ).astype(BF)

    class Scatter:
        def __init__(self, partial, core, far, near):
            self.partial, self.core, self.far, self.near = partial, core, far, near
            self.over = []
            for dy in (2, 1, 3, 0):
                there = lax.rem(y + dy, 4)
                self.over.append((dy, Link(slot(partial, dy, 1 - c), core.at[there], partner).start()))
            always.extend(link for _, link in self.over)

        def combine(self):
            partial, core = self.partial, self.core
            for dy, link in self.over:
                there = lax.rem(y + dy, 4)
                link.got(core.at[there])
                if dy == 0:
                    continue
                rows = pl.ds(aligned((there * 2 + c) * TOK, TOK), TOK)
                partial[rows] = (partial[rows].astype(F32) + core[there].astype(F32)).astype(BF)
                if dy == 2:
                    self.t0 = Link(slot(partial, 2, c, 0, 64), self.far.at[0], y_dev(1)).start()
                    self.t1 = Link(slot(partial, 2, c, 64, 64), self.far.at[1], y_dev(3)).start()
                elif dy == 1:
                    self.t2 = Link(slot(partial, 1, c, 64, 64), self.near.at[0, pl.ds(64, 64)], y_dev(1)).start()
                else:
                    self.t3 = Link(slot(partial, 3, c, 0, 64), self.near.at[1, pl.ds(0, 64)], y_dev(3)).start()
            always.extend([self.t0, self.t1, self.t2, self.t3])

        def middle(self):
            partial, far = self.partial, self.far
            for dy, lo, k, link in ((1, 0, 0, self.t0), (3, 64, 1, self.t1)):
                link.got(far.at[k])
                there = lax.rem(y + dy, 4)
                rows = pl.ds(aligned((there * 2 + c) * TOK + lo, 16), 64)
                partial[rows] = (partial[rows].astype(F32) + far[k].astype(F32)).astype(BF)
                onward = Link(slot(partial, dy, c, lo, 64), self.near.at[k, pl.ds(lo, 64)], y_dev(dy)).start()
                always.append(onward)
                if k == 0:
                    self.t4 = onward
                else:
                    self.t5 = onward

        def finish(self):
            near = self.near
            self.t2.got(near.at[0, pl.ds(64, 64)])
            self.t3.got(near.at[1, pl.ds(0, 64)])
            self.t4.got(near.at[0, pl.ds(0, 64)])
            self.t5.got(near.at[1, pl.ds(64, 64)])
            own = self.partial[own_rows].astype(F32) + self.core[y].astype(F32)
            return own + near[0].astype(F32) + near[1].astype(F32)

    across(slope, up_all, part_back)
    sc_back = Scatter(part_back, core_back, far_back, near_back)

    @pl.when(not_owner)
    def _():
        red_down.middle(1)
        red_up.send_near(1)

    across(act, down_all, part_out)
    sc_out = Scatter(part_out, core_out, far_out, near_out)
    sc_back.combine()

    @pl.when(not_owner)
    def _():
        red_up.middle(0)

    sc_back.middle()
    sc_out.combine()

    @pl.when(not_owner)
    def _():
        red_up.middle(1)

    back[...] = sc_back.finish()
    standard, inverse = spread()
    nb = back[...]
    rows_small = (
        (0, D // 128, jnp.sum(nb * standard, axis=0, keepdims=True)),
        (D // 128, D // 128, jnp.sum(nb, axis=0, keepdims=True)),
        (2 * (D // 128), HID // 128, bias_sum[...]),
    )
    small[...] = jnp.zeros_like(small)
    for first, length, row in rows_small:
        for i in range(length):
            small[first + i : first + i + 1, :] = row[:, 128 * i : 128 * (i + 1)]
    n_norm = 2 * (D // 128)
    small_over = Link(small, small_core, partner).start()
    always.append(small_over)
    scaled = nb * gain[...][None]
    back[...] = inverse * (
        scaled
        - jnp.mean(scaled, axis=1, keepdims=True)
        - standard * jnp.mean(scaled * standard, axis=1, keepdims=True)
    )
    put_back = pltpu.make_async_copy(back, out_back, local_sems.at[0])
    put_back.start()

    def load_own(rows, source):
        for k in range(8):
            j, lanes = k % 4, slice((k // 4) * CHUNK_COLS, (k // 4 + 1) * CHUNK_COLS)
            total = source(j, rows, lanes).astype(F32)
            total = total + near_a[j, rows, lanes].astype(F32) + near_b[j, rows, lanes].astype(F32)
            zsum[k, rows] = total.astype(BF)

    def at_z(d):
        return lax.rem(z + d, 8)

    def add_rows(k, rows, incoming):
        zsum[k, rows] = (zsum[k, rows].astype(F32) + incoming.astype(F32)).astype(BF)

    overs = []

    def along_z(u):
        rows = UNITS[u]
        head, tail = pl.ds(rows.start, 48), pl.ds(rows.start + 48, rows.size - 48)

        @pl.when(owner)
        def _():
            red_down.finish(u)
            load_own(rows, lambda j, rows, lanes: grad_down[h_me * 4 + j, rows, lanes])

        @pl.when(not_owner)
        def _():
            if u == 0:
                own_link.got(own_up)
            red_up.finish(u)
            load_own(rows, lambda j, rows, lanes: own_up[j, rows, lanes])

        def link(src, dst, device):
            made = Link(src, dst, device).start()
            always.append(made)
            return made

        f = link(zsum.at[at_z(4), head], z_near_a.at[0, head], z_dev(1))
        b = link(zsum.at[at_z(4), tail], z_near_b.at[0, tail], z_dev(7))
        yield
        for step in range(3):
            got_f, got_b = (head, tail) if step == 0 else (rows, rows)
            f.got(z_near_a.at[step, got_f])
            add_rows(at_z(3 - step), got_f, z_near_a[step, got_f])
            f = link(zsum.at[at_z(3 - step), rows], z_near_a.at[step + 1, rows], z_dev(1))
            b.got(z_near_b.at[step, got_b])
            add_rows(at_z(5 + step), got_b, z_near_b[step, got_b])
            b = link(zsum.at[at_z(5 + step), rows], z_near_b.at[step + 1, rows], z_dev(7))
            yield
        f.got(z_near_a.at[3, rows])
        b.got(z_near_b.at[3, rows])
        mine[z, rows] = (
            zsum[z, rows].astype(F32) + z_near_a[3, rows].astype(F32) + z_near_b[3, rows].astype(F32)
        ).astype(BF)

        def forward(k, rows, device):
            return link(mine.at[k, rows], mine.at[k, rows], device)

        def hand_over(k):
            overs.append((link(mine.at[k, rows], other.at[k, rows], partner), k, rows))

        f, b = forward(z, rows, z_dev(1)), forward(z, rows, z_dev(7))
        hand_over(z)
        yield
        for d in (1, 2, 3):
            f.got(mine.at[at_z(8 - d), rows])
            f = forward(at_z(8 - d), rows if d < 3 else head, z_dev(1))
            b.got(mine.at[at_z(d), rows])
            b = forward(at_z(d), rows if d < 3 else tail, z_dev(7))
            hand_over(at_z(8 - d))
            hand_over(at_z(d))
            yield
        f.got(mine.at[at_z(4), head])
        b.got(mine.at[at_z(4), tail])
        hand_over(at_z(4))
        yield

    def small_sums():
        small_over.got(small_core)
        keep = lax.broadcasted_iota(jnp.int32, small.shape, 0) < n_norm
        small_y[y] = small[...] + jnp.where(keep, small_core[...], 0.0)
        y_links = [Link(small_y.at[y], small_y.at[y], y_dev(d)).start() for d in (1, 2, 3)]
        yield
        for d, link in zip((1, 2, 3), y_links):
            link.got(small_y.at[lax.rem(y + 4 - d, 4)])
        ysum = small_y[0] + small_y[1] + small_y[2] + small_y[3]
        small_x[x] = jnp.where(keep, ysum, small[...])
        x_links = [Link(small_x.at[x], small_x.at[x], x_dev(d)).start() for d in (1, 2, 3)]
        yield
        for d, link in zip((1, 2, 3), x_links):
            link.got(small_x.at[lax.rem(x + 4 - d, 4)])
        small_z[z] = small_x[0] + small_x[1] + small_x[2] + small_x[3]
        z_links = [Link(small_z.at[z], small_z.at[z], z_dev(d)).start() for d in range(1, 8)]
        yield
        for d, link in zip(range(1, 8), z_links):
            link.got(small_z.at[at_z(8 - d)])
        total = small_z[0]
        for k in range(1, 8):
            total = total + small_z[k]
        small_total[0] = total
        last = Link(small_total.at[0], small_total.at[1], partner).start()
        always.extend([*y_links, *x_links, *z_links, last])
        yield
        last.got(small_total.at[1])
        yield

    first, second, sums = along_z(0), along_z(1), small_sums()
    next(first)
    next(sums)
    next(first)
    next(sums)
    sc_out.middle()
    next(first)
    next(sums)
    next(second)
    next(first)
    next(second)
    next(sums)
    next(first)
    next(second)
    next(first)
    next(second)
    next(sums)
    put_small = pltpu.make_async_copy(small_total, out_small, local_sems.at[4])
    put_small.start()
    next(first)
    next(second)
    proj[...] = sc_out.finish() + down_bias[...][None]
    put_proj = pltpu.make_async_copy(proj, out_proj, local_sems.at[1])
    put_proj.start()
    next(first)
    next(second)
    next(first)
    next(second)
    next(second)
    next(second)
    put_mine = pltpu.make_async_copy(mine, out_mine, local_sems.at[2])
    put_mine.start()
    for link, k, rows in overs:
        link.got(other.at[k, rows])
    put_other = pltpu.make_async_copy(other, out_other, local_sems.at[3])
    put_other.start()

    for link in always:
        link.sent()

    @pl.when(owner)
    def _():
        for link in when_owner:
            link.sent()

    @pl.when(jnp.logical_not(owner))
    def _():
        for link in when_relay:
            link.sent()

    for put in (put_back, put_proj, put_mine, put_other, put_small):
        put.wait()
    assert count[0] <= N_LINKS


N_LINKS = 192


def on_device(patches, norm_gain, norm_bias, up_weight, up_bias, down_weight, down_bias, cotangent):
    scaling = 1.0 / math.sqrt(TOK * 256)
    vmem = pl.BlockSpec(memory_space=pltpu.VMEM)
    hbm = pl.BlockSpec(memory_space=pl.ANY)

    def V(*shape, dtype=BF):
        return pltpu.VMEM(shape, dtype)

    proj, back, mine, other, small = pl.pallas_call(
        step_kernel,
        out_shape=(
            jax.ShapeDtypeStruct((TOK, D), F32),
            jax.ShapeDtypeStruct((TOK, D), F32),
            jax.ShapeDtypeStruct((8, CHUNK_ROWS, CHUNK_COLS), BF),
            jax.ShapeDtypeStruct((8, CHUNK_ROWS, CHUNK_COLS), BF),
            jax.ShapeDtypeStruct((2, 32, 128), F32),
        ),
        in_specs=[hbm, hbm, vmem, vmem, vmem, vmem, hbm, hbm],
        out_specs=[hbm] * 5,
        scratch_shapes=[
            V(TOK, D), V(GROUP, D), V(GROUP, D), V(D, HID), V(D, HID), V(HID, dtype=F32),
            V(GROUP, HID, dtype=F32), V(GROUP, HID), V(GROUP, HID),
            V(GROUP, D), V(GROUP, D), V(4, TOK, D), V(4, TOK, D),
            V(2, 64, D), V(2, 64, D), V(2, TOK, D), V(2, TOK, D),
            V(8, CHUNK_ROWS, HID), V(8, CHUNK_ROWS, HID), V(4, CHUNK_ROWS, HID), V(4, CHUNK_ROWS, HID),
            V(4, CHUNK_ROWS, HID), V(4, CHUNK_ROWS, HID), V(4, CHUNK_ROWS, HID),
            V(8, CHUNK_ROWS, CHUNK_COLS), V(4, CHUNK_ROWS, CHUNK_COLS), V(4, CHUNK_ROWS, CHUNK_COLS),
            V(8, CHUNK_ROWS, CHUNK_COLS), V(8, CHUNK_ROWS, CHUNK_COLS),
            V(TOK, D, dtype=F32), V(TOK, D, dtype=F32), V(1, HID, dtype=F32),
            V(32, 128, dtype=F32), V(32, 128, dtype=F32), V(4, 32, 128, dtype=F32),
            V(4, 32, 128, dtype=F32), V(8, 32, 128, dtype=F32), V(2, 32, 128, dtype=F32),
            pltpu.SemaphoreType.DMA((N_LINKS,)),
            pltpu.SemaphoreType.DMA((N_LINKS,)),
            pltpu.SemaphoreType.DMA((9,)),
        ],
        compiler_params=pltpu.CompilerParams(
            collective_id=0, has_side_effects=True, vmem_limit_bytes=63 * 1024 * 1024
        ),
    )(
        patches, cotangent, norm_gain, norm_bias, up_bias, down_bias,
        up_weight, down_weight.T,
    )

    owner = lax.axis_index("row_0") == lax.axis_index("dp_1")

    def whole(chunks):
        left, right = chunks.reshape(2, HALF, CHUNK_COLS)
        return jnp.concatenate([left, right], axis=1).astype(F32) * scaling

    up_grad = whole(jnp.where(owner, other, mine))
    down_grad = whole(jnp.where(owner, mine, other)).T
    small = small * scaling
    n = D // 128
    norm_grad = small[0, : 2 * n].reshape(2, D)
    bias_grad = jnp.where(owner, small[0], small[1])[2 * n : 2 * n + HID // 128].reshape(HID)
    output = proj + patches.astype(F32)
    patch_grad = back + cotangent.astype(F32)
    return output, patch_grad, up_grad, down_grad, bias_grad, norm_grad


def solution(mesh):
    split = Mesh(
        mesh.devices.reshape(8, 2, 2, 4, mesh.shape["col"]),
        ("dp_0", "dp_1", "row_0", "row_1", "col"),
    )
    return jax.shard_map(
        on_device,
        mesh=split,
        in_specs=(
            P(DP_ROW_COL, None), P(), P(), P("col", ROW), P(ROW), P(ROW, "col"), P(), P(DP_ROW_COL, None),
        ),
        out_specs=(
            P(DP_ROW_COL, None), P(DP_ROW_COL, None), P("col", ROW), P(ROW, "col"), P(ROW), P(),
        ),
        check_vma=False,
    )
```

```python
import math

import jax
import jax.numpy as jnp
from jax import lax
from jax.experimental import pallas as pl
from jax.experimental.pallas import tpu as pltpu
from jax.sharding import Mesh
from jax.sharding import PartitionSpec as P

MESH = pl.DeviceIdType.MESH
ROW = ("row_0", "row_1")
DP_ROW_COL = ("dp_0", "dp_1", "row_0", "row_1", "col")

EPSILON = 1e-06
GELU_ROOT = 0.7978845608028654
GELU_CUBIC = 0.044715

D = 1408
HALF = 704
QUARTER = 352
HID = 768
TOK = 128
GROUP = 1024
CHUNK_ROWS, CHUNK_COLS = 176, 384
UNITS = (pl.ds(0, 96), pl.ds(96, 80))
BF = jnp.bfloat16
F32 = jnp.float32


def aligned(value, tile):
    return pl.multiple_of(value, tile)


def step_kernel(
    patches_in, cotangent_in, gain, bias, up_bias, down_bias, up, down,
    out_proj, out_back, out_mine, out_other, out_small,
    patches, normed, cot, up_all, down_all, bias_all, gelu_d, act, slope,
    part_out, part_back, core_out, core_back, far_out, far_back, near_out, near_back,
    grad_up, grad_down, swap_up, half_up, far_up, far_down, own_up, near_a, near_b, near_ua, near_ub,
    zsum, usum, z_near_a, z_near_b, mine, other,
    proj, back, bias_sum, small, small_core, small_y, small_x, small_z, small_total,
    send_sems, recv_sems, local_sems, put_sems,
):
    z, c = lax.axis_index("dp_0"), lax.axis_index("dp_1")
    xl, y, xh = lax.axis_index("row_0"), lax.axis_index("row_1"), lax.axis_index("col")
    x = xh * 2 + xl
    owner = xl == c

    def x_dev(d, swap=False):
        there = lax.rem(x + d, 4)
        place = {"row_0": lax.rem(there, 2), "col": lax.div(there, 2)}
        return {**place, "dp_1": 1 - c} if swap else place

    def y_dev(d):
        return {"row_1": lax.rem(y + d, 4)}

    def z_dev(d):
        return {"dp_0": lax.rem(z + d, 8)}

    partner = {"dp_1": 1 - c}
    peers = [partner]
    peers += [x_dev(d) for d in (1, 2, 3)] + [x_dev(d, True) for d in (1, 3)]
    peers += [y_dev(d) for d in (1, 2, 3)] + [z_dev(d) for d in range(1, 8)]
    own_rows = pl.ds(aligned((y * 2 + c) * TOK, TOK), TOK)
    own_block = pl.ds(aligned(xh * HALF, 16), HALF)
    load_patches = pltpu.make_async_copy(patches_in, patches, local_sems.at[5])
    load_cot = pltpu.make_async_copy(cotangent_in, cot.at[own_rows], local_sems.at[6])
    load_up = pltpu.make_async_copy(up, up_all.at[own_block], local_sems.at[7])
    load_down = pltpu.make_async_copy(down, down_all.at[own_block], local_sems.at[8])
    load_patches.start()
    load_cot.start()

    @pl.when(owner)
    def _():
        load_up.start()
        load_down.start()

    barrier = pltpu.get_barrier_semaphore()
    for peer in peers:
        pl.semaphore_signal(barrier, inc=1, device_id=peer, device_id_type=MESH)
    def spread():
        wide = patches[...].astype(F32)
        centred = wide - jnp.mean(wide, axis=1, keepdims=True)
        inverse = lax.rsqrt(jnp.mean(centred * centred, axis=1, keepdims=True) + EPSILON)
        return centred * inverse, inverse

    load_patches.wait()
    normed[own_rows] = (spread()[0] * gain[...][None] + bias[...][None]).astype(BF)
    load_cot.wait()
    pl.semaphore_wait(barrier, len(peers))

    count = [0]

    class Link:
        def __init__(self, src, dst, device):
            self.k = count[0]
            count[0] += 1
            self.copy = pltpu.make_async_remote_copy(
                src_ref=src, dst_ref=dst, send_sem=send_sems.at[self.k], recv_sem=recv_sems.at[self.k],
                device_id=device, device_id_type=MESH,
            )

        def start(self):
            self.copy.start()
            return self

        def sent(self):
            self.copy.wait_send()

        def got(self, dst):
            pltpu.make_async_remote_copy(
                src_ref=dst, dst_ref=dst, send_sem=send_sems.at[self.k], recv_sem=recv_sems.at[self.k],
                device_id=partner, device_id_type=MESH,
            ).wait_recv()

    always, when_owner, when_relay = [], [], []

    h_me = xh
    h_next = lax.div(lax.rem(x + 1, 4), 2)
    h_prev = lax.div(lax.rem(x + 3, 4), 2)

    lanes_x = pl.ds(aligned(lax.rem(z, 2) * CHUNK_COLS, 128), CHUNK_COLS)
    lanes_z = pl.ds(aligned((1 - lax.rem(z, 2)) * CHUNK_COLS, 128), CHUNK_COLS)

    def part(ref, h, first, lanes):
        start = aligned(h * HALF + (0 if first else QUARTER), 16)
        return ref.at[pl.ds(start, QUARTER), lanes]

    class Gather:
        def __init__(self, whole):
            def link(h, first, device):
                return Link(part(whole, h, first, lanes_x), part(whole, h, first, lanes_x), device)

            self.whole = whole
            self.a1, self.b2 = link(h_me, True, x_dev(1)), link(h_me, False, x_dev(3))
            self.b1, self.a2 = link(h_me, False, x_dev(1)), link(h_me, True, x_dev(3))
            self.ra, self.rb = link(h_prev, True, x_dev(1)), link(h_next, False, x_dev(3))
            self.oa, self.ob = link(1 - h_me, True, z_dev(1)), link(1 - h_me, False, z_dev(7))
            self.pa, self.nb = link(h_prev, True, z_dev(1)), link(h_next, False, z_dev(7))
            self.pb, self.na = link(h_prev, False, z_dev(7)), link(h_next, True, z_dev(1))
            when_owner.extend([self.a1, self.b2, self.b1, self.a2, self.oa, self.ob])
            when_relay.extend([self.ra, self.rb, self.pa, self.nb, self.pb, self.na])

        def here(self, h, first):
            return part(self.whole, h, first, lanes_x)

        def there(self, h, first):
            return part(self.whole, h, first, lanes_z)

        def begin(self):
            for link in (self.a1, self.b2, self.b1, self.a2):
                link.start()

        def relay(self):
            self.a1.got(self.here(h_prev, True))
            self.ra.start()
            self.pa.start()
            self.b2.got(self.here(h_next, False))
            self.rb.start()
            self.nb.start()

        def relay_last(self):
            self.b1.got(self.here(h_prev, False))
            self.pb.start()
            self.a2.got(self.here(h_next, True))
            self.na.start()

        def pass_on(self):
            self.ra.got(self.here(1 - h_me, True))
            self.oa.start()
            self.rb.got(self.here(1 - h_me, False))
            self.ob.start()

        def finish(self):
            @pl.when(owner)
            def _():
                self.oa.got(self.there(1 - h_me, True))
                self.ob.got(self.there(1 - h_me, False))

            @pl.when(jnp.logical_not(owner))
            def _():
                self.pa.got(self.there(h_prev, True))
                self.nb.got(self.there(h_next, False))
                self.pb.got(self.there(h_prev, False))
                self.na.got(self.there(h_next, True))

    ups, downs = Gather(up_all), Gather(down_all)
    bias_link = Link(up_bias, bias_all, x_dev(1))
    when_owner.append(bias_link)

    @pl.when(owner)
    def _():
        load_up.wait()
        ups.begin()
        bias_link.start()
        load_down.wait()
        downs.begin()
        bias_all[...] = up_bias[...]

    def slot(ref, dy, core, lo=0, rows=TOK):
        there = lax.rem(y + dy, 4)
        return ref.at[pl.ds(aligned((there * 2 + core) * TOK + lo, 16), rows)]

    class Tokens:
        def __init__(self, own, whole):
            self.whole = whole
            self.next = Link(own, slot(whole, 0, c), y_dev(1)).start()
            self.prev = Link(own, slot(whole, 0, c), y_dev(3)).start()
            self.over = Link(own, slot(whole, 0, c), partner).start()
            always.extend([self.next, self.prev, self.over])

        def relay(self):
            whole = self.whole
            self.next.got(slot(whole, 3, c))
            self.far_a = Link(slot(whole, 3, c, 0, 64), slot(whole, 3, c, 0, 64), y_dev(1)).start()
            self.over_a = Link(slot(whole, 3, c), slot(whole, 3, c), partner).start()
            self.prev.got(slot(whole, 1, c))
            self.far_b = Link(slot(whole, 1, c, 64, 64), slot(whole, 1, c, 64, 64), y_dev(3)).start()
            self.over_b = Link(slot(whole, 1, c), slot(whole, 1, c), partner).start()
            always.extend([self.far_a, self.over_a, self.far_b, self.over_b])

        def far(self):
            whole = self.whole
            self.far_a.got(slot(whole, 2, c, 0, 64))
            self.far_b.got(slot(whole, 2, c, 64, 64))
            self.over_far = Link(slot(whole, 2, c), slot(whole, 2, c), partner).start()
            always.append(self.over_far)

        def from_partner(self, dy):
            name = ("over", "over_b", "over_far", "over_a")[dy]
            getattr(self, name).got(slot(self.whole, dy, 1 - c))

    tok_n = Tokens(normed.at[own_rows], normed)
    tok_c = Tokens(cot.at[own_rows], cot)

    @pl.when(jnp.logical_not(owner))
    def _():
        ups.relay()

    tok_n.relay()

    @pl.when(owner)
    def _():
        ups.pass_on()

    @pl.when(jnp.logical_not(owner))
    def _():
        bias_link.got(bias_all)
        ups.relay_last()
        downs.relay()

    tok_c.relay()

    @pl.when(owner)
    def _():
        downs.pass_on()

    @pl.when(jnp.logical_not(owner))
    def _():
        downs.relay_last()

    def rows_of(dy):
        return pl.ds(aligned(lax.rem(y + dy, 4) * 256, 256), 256)

    def forward_block(dy):
        rows = rows_of(dy)
        v = jnp.dot(normed[rows], up_all[...], preferred_element_type=F32) + bias_all[...][None]
        inner = jnp.tanh(GELU_ROOT * (v + GELU_CUBIC * v * v * v))
        act[rows] = (0.5 * v * (1.0 + inner)).astype(BF)
        gelu_d[rows] = 0.5 * (1.0 + inner) + 0.5 * v * (1.0 - inner * inner) * GELU_ROOT * (
            1.0 + 3.0 * GELU_CUBIC * v * v
        )

    def slope_block(dy):
        rows = rows_of(dy)
        s = jnp.dot(cot[rows], down_all[...], preferred_element_type=F32) * gelu_d[rows]
        s = s.astype(BF)
        slope[rows] = s
        bias_sum[...] += jnp.sum(s.astype(F32), axis=0, keepdims=True)

    ups.finish()
    tok_n.far()
    for dy in (0, 3, 1):
        tok_n.from_partner(dy)

    @pl.loop(0, 3)
    def _(i):
        forward_block(lax.rem(i + 3, 4))

    tok_c.far()
    tok_n.from_partner(2)
    forward_block(2)

    downs.finish()
    bias_sum[...] = jnp.zeros_like(bias_sum)
    for dy in (0, 3, 1):
        tok_c.from_partner(dy)

    @pl.loop(0, 3)
    def _(i):
        slope_block(lax.rem(i + 3, 4))

    tok_c.from_partner(2)

    def outer(left, right, result):
        for lo, hi in ((0, 512), (512, 1024), (1024, D)):
            block = lax.dot_general(
                left[:, lo:hi], right[...], (((0,), (0,)), ((), ())), preferred_element_type=F32
            ).astype(BF)
            while lo < hi:
                j, r = divmod(lo, CHUNK_ROWS)
                rows = min(CHUNK_ROWS - r, hi - lo)
                result[j, r : r + rows] = block[:rows]
                block, lo = block[rows:], lo + rows

    class Reduce:
        def __init__(self, grad, far, near_a, near_b, swap):
            self.grad, self.far, self.near, self.links = grad, far, (near_a, near_b), []
            lo, hi = pl.ds(0, 2), pl.ds(2, 2)
            for rows in UNITS:
                s0 = Link(self.of(1 - h_me, True, rows), far.at[lo, rows], x_dev(1))
                s1 = Link(self.of(1 - h_me, False, rows), far.at[hi, rows], x_dev(3))
                s2 = Link(self.of(h_next, False, rows), near_a.at[hi, rows], x_dev(1, swap))
                s4 = Link(self.of(h_prev, True, rows), near_b.at[lo, rows], x_dev(3, swap))
                s3 = Link(self.of(h_next, True, rows), near_a.at[lo, rows], x_dev(1, swap))
                s5 = Link(self.of(h_prev, False, rows), near_b.at[hi, rows], x_dev(3, swap))
                when_owner.extend([s0, s1])
                when_relay.extend([s2, s4, s3, s5])
                self.links.append((s0, s1, s2, s3, s4, s5))

        def of(self, h, first, rows):
            return self.grad.at[pl.ds(h * 4 + (0 if first else 2), 2), rows]

        def send_far(self, u):
            s0, s1, _, _, _, _ = self.links[u]
            s0.start()
            s1.start()

        def send_near(self, u):
            _, _, s2, _, s4, _ = self.links[u]
            s2.start()
            s4.start()

        def middle(self, u):
            grad, far, rows = self.grad, self.far, UNITS[u]
            s0, s1, _, s3, _, s5 = self.links[u]
            for link, onward, h, first, k in ((s0, s3, h_next, True, 0), (s1, s5, h_prev, False, 2)):
                link.got(far.at[pl.ds(k, 2), rows])
                for j in (0, 1):
                    at = h * 4 + (0 if first else 2) + j
                    grad[at, rows] = (grad[at, rows].astype(F32) + far[k + j, rows].astype(F32)).astype(BF)
                onward.start()

        def finish(self, u):
            _, _, s2, s3, s4, s5 = self.links[u]
            lo, hi, rows = pl.ds(0, 2), pl.ds(2, 2), UNITS[u]
            near_a, near_b = self.near
            s2.got(near_a.at[hi, rows])
            s4.got(near_b.at[lo, rows])
            s3.got(near_a.at[lo, rows])
            s5.got(near_b.at[hi, rows])

    red_down = Reduce(grad_down, far_down, near_a, near_b, False)
    red_up = Reduce(half_up, far_up, near_ua, near_ub, True)
    own_links = []
    for rows in UNITS:
        own_links.append(Link(half_up.at[pl.ds(h_me * 4, 4), rows], own_up.at[pl.ds(0, 4), rows], partner))
    when_owner.extend(own_links)
    not_owner = jnp.logical_not(owner)

    outer(cot, act, grad_down)

    @pl.when(owner)
    def _():
        red_down.send_far(0)
        red_down.send_far(1)

    @pl.when(not_owner)
    def _():
        red_down.send_near(0)

    slope_block(2)
    outer(normed, slope, grad_up)

    swaps = []
    for rows in UNITS:
        pair = []
        for h, d in ((0, 1), (1, 7)):
            tiles = pl.ds(h * 4, 4)
            pair.append(Link(grad_up.at[tiles, rows, lanes_z], swap_up.at[tiles, rows], z_dev(d)).start())
        swaps.append(pair)
        always.extend(pair)

    def swapped(u):
        rows = UNITS[u]
        for h, swap in enumerate(swaps[u]):
            swap.got(swap_up.at[pl.ds(h * 4, 4), rows])
        for k in range(8):
            half_up[k, rows] = (grad_up[k, rows, lanes_x].astype(F32) + swap_up[k, rows].astype(F32)).astype(BF)

        @pl.when(owner)
        def _():
            own_links[u].start()
            red_up.send_far(u)

    def at_z(d):
        return lax.rem(z + d, 8)

    def add_rows(sums, k, rows, incoming):
        sums[k, rows] = (sums[k, rows].astype(F32) + incoming.astype(F32)).astype(BF)

    def link(src, dst, device):
        made = Link(src, dst, device).start()
        always.append(made)
        return made

    def held(src, dst, device, when):
        made = Link(src, dst, device)
        when.append(made)
        return made

    puts = []

    class AlongZ:
        def __init__(self, u):
            self.u, self.rows = u, UNITS[u]
            rows = self.rows
            self.head = pl.ds(rows.start, 48)
            self.tail = pl.ds(rows.start + 48, rows.size - 48)
            self.down = []
            for step in range(4):
                f, b = (self.head, self.tail) if step == 0 else (rows, rows)
                self.down.append((
                    held(zsum.at[at_z(4 - step), f], z_near_a.at[step, f], z_dev(1), when_owner),
                    held(zsum.at[at_z(4 + step), b], z_near_b.at[step, b], z_dev(7), when_owner),
                ))
            self.up = []
            for step in range(2):
                f, b = (self.head, self.tail) if step == 0 else (rows, rows)
                to, fro = lax.div(at_z(4 - 2 * step), 2), lax.div(at_z(4 + 2 * step), 2)
                self.up.append((
                    held(usum.at[to, f], z_near_a.at[step, f], z_dev(2), when_relay),
                    held(usum.at[fro, b], z_near_b.at[step, b], z_dev(6), when_relay),
                ))
            self.out = [
                held(mine.at[z, rows], mine.at[z, rows], z_dev(1), always),
                held(mine.at[z, rows], mine.at[z, rows], z_dev(7), always),
                held(mine.at[z, rows], other.at[z, rows], partner, always),
            ]

        def begin_down(self):
            red_down.finish(self.u)
            for k in range(8):
                j, lanes = k // 2, slice((k % 2) * CHUNK_COLS, (k % 2 + 1) * CHUNK_COLS)
                total = grad_down[h_me * 4 + j, self.rows, lanes].astype(F32)
                total = total + near_a[j, self.rows, lanes].astype(F32) + near_b[j, self.rows, lanes].astype(F32)
                zsum[k, self.rows] = total.astype(BF)
            for started in self.down[0]:
                started.start()

        def step_down(self, step):
            got_f, got_b = (self.head, self.tail) if step == 0 else (self.rows, self.rows)
            f, b = self.down[step]
            f.got(z_near_a.at[step, got_f])
            add_rows(zsum, at_z(3 - step), got_f, z_near_a[step, got_f])
            self.down[step + 1][0].start()
            b.got(z_near_b.at[step, got_b])
            add_rows(zsum, at_z(5 + step), got_b, z_near_b[step, got_b])
            self.down[step + 1][1].start()

        def begin_up(self):
            own_links[self.u].got(own_up.at[pl.ds(0, 4), self.rows])
            red_up.finish(self.u)
            for j in range(4):
                total = own_up[j, self.rows].astype(F32)
                total = total + near_ua[j, self.rows].astype(F32) + near_ub[j, self.rows].astype(F32)
                usum[j, self.rows] = total.astype(BF)
            for started in self.up[0]:
                started.start()

        def step_up(self):
            f, b = self.up[0]
            f.got(z_near_a.at[0, self.head])
            add_rows(usum, lax.div(at_z(2), 2), self.head, z_near_a[0, self.head])
            self.up[1][0].start()
            b.got(z_near_b.at[0, self.tail])
            add_rows(usum, lax.div(at_z(6), 2), self.tail, z_near_b[0, self.tail])
            self.up[1][1].start()

        def end(self, sums, at, links, k):
            rows = self.rows
            f, b = links
            f.got(z_near_a.at[k, rows])
            b.got(z_near_b.at[k, rows])
            mine[z, rows] = (
                sums[at, rows].astype(F32) + z_near_a[k, rows].astype(F32) + z_near_b[k, rows].astype(F32)
            ).astype(BF)
            for started in self.out:
                started.start()

        def end_down(self):
            self.end(zsum, z, self.down[3], 3)

        def end_up(self):
            self.end(usum, lax.div(z, 2), self.up[1], 1)

        def put(self, chunks, result, k):
            row = lax.div(k, 2) * CHUNK_ROWS + self.rows.start
            lane = lax.rem(k, 2) * CHUNK_COLS
            there = result.at[pl.ds(aligned(row, 16), self.rows.size), pl.ds(aligned(lane, 128), CHUNK_COLS)]
            copy = pltpu.make_async_copy(chunks.at[k, self.rows], there, put_sems.at[len(puts)])
            copy.start()
            puts.append(copy)

        def spread(self):
            rows = self.rows
            overs = [(self.out[2], z)]
            f, b = self.out[:2]
            self.put(mine, out_mine, z)

            def pass_on(k, rows, device):
                return link(mine.at[k, rows], mine.at[k, rows], device)

            def hand_over(k):
                overs.append((link(mine.at[k, rows], other.at[k, rows], partner), k))

            def take_over(count):
                for _ in range(count):
                    sent, k = overs.pop(0)
                    sent.got(other.at[k, rows])
                    self.put(other, out_other, k)

            for d in (1, 2, 3):
                f.got(mine.at[at_z(8 - d), rows])
                f = pass_on(at_z(8 - d), rows if d < 3 else self.head, z_dev(1))
                b.got(mine.at[at_z(d), rows])
                b = pass_on(at_z(d), rows if d < 3 else self.tail, z_dev(7))
                hand_over(at_z(8 - d))
                hand_over(at_z(d))
                self.put(mine, out_mine, at_z(8 - d))
                self.put(mine, out_mine, at_z(d))
                yield
            f.got(mine.at[at_z(4), self.head])
            b.got(mine.at[at_z(4), self.tail])
            hand_over(at_z(4))
            self.put(mine, out_mine, at_z(4))
            take_over(5)
            yield
            take_over(3)
            yield

    unit0, unit1 = AlongZ(0), AlongZ(1)

    def across(left, right, result):
        @pl.loop(0, GROUP // 256)
        def _(i):
            rows = pl.ds(aligned(i * 256, 256), 256)
            result[rows] = lax.dot_general(
                left[rows], right[...], (((1,), (1,)), ((), ())), preferred_element_type=F32
            ).astype(BF)

    class Scatter:
        def __init__(self, partial, core, far, near):
            self.partial, self.core, self.far, self.near = partial, core, far, near
            self.over = []
            for dy in (2, 1, 3, 0):
                there = lax.rem(y + dy, 4)
                self.over.append((dy, Link(slot(partial, dy, 1 - c), core.at[there], partner).start()))
            always.extend(link for _, link in self.over)

        def combine(self):
            partial, core = self.partial, self.core
            for dy, link in self.over:
                there = lax.rem(y + dy, 4)
                link.got(core.at[there])
                if dy == 0:
                    continue
                rows = pl.ds(aligned((there * 2 + c) * TOK, TOK), TOK)
                partial[rows] = (partial[rows].astype(F32) + core[there].astype(F32)).astype(BF)
                if dy == 2:
                    self.t0 = Link(slot(partial, 2, c, 0, 64), self.far.at[0], y_dev(1)).start()
                    self.t1 = Link(slot(partial, 2, c, 64, 64), self.far.at[1], y_dev(3)).start()
                elif dy == 1:
                    self.t2 = Link(slot(partial, 1, c, 64, 64), self.near.at[0, pl.ds(64, 64)], y_dev(1)).start()
                else:
                    self.t3 = Link(slot(partial, 3, c, 0, 64), self.near.at[1, pl.ds(0, 64)], y_dev(3)).start()
            always.extend([self.t0, self.t1, self.t2, self.t3])

        def middle(self):
            partial, far = self.partial, self.far
            for dy, lo, k, link in ((1, 0, 0, self.t0), (3, 64, 1, self.t1)):
                link.got(far.at[k])
                there = lax.rem(y + dy, 4)
                rows = pl.ds(aligned((there * 2 + c) * TOK + lo, 16), 64)
                partial[rows] = (partial[rows].astype(F32) + far[k].astype(F32)).astype(BF)
                onward = Link(slot(partial, dy, c, lo, 64), self.near.at[k, pl.ds(lo, 64)], y_dev(dy)).start()
                always.append(onward)
                if k == 0:
                    self.t4 = onward
                else:
                    self.t5 = onward

        def finish(self):
            near = self.near
            self.t2.got(near.at[0, pl.ds(64, 64)])
            self.t3.got(near.at[1, pl.ds(0, 64)])
            self.t4.got(near.at[0, pl.ds(0, 64)])
            self.t5.got(near.at[1, pl.ds(64, 64)])
            own = self.partial[own_rows].astype(F32) + self.core[y].astype(F32)
            return own + near[0].astype(F32) + near[1].astype(F32)

    across(slope, up_all, part_back)
    sc_back = Scatter(part_back, core_back, far_back, near_back)


    @pl.when(not_owner)
    def _():
        red_down.middle(0)
        red_down.send_near(1)

    across(act, down_all, part_out)
    sc_out = Scatter(part_out, core_out, far_out, near_out)

    swapped(0)

    @pl.when(not_owner)
    def _():
        red_up.send_near(0)

    sc_back.combine()

    @pl.when(not_owner)
    def _():
        red_down.middle(1)

    swapped(1)

    @pl.when(owner)
    def _():
        unit0.begin_down()

    sc_back.middle()

    @pl.when(owner)
    def _():
        unit0.step_down(0)

    sc_out.combine()

    @pl.when(owner)
    def _():
        unit1.begin_down()
        unit0.step_down(1)
        unit1.step_down(0)
        unit0.step_down(2)

    @pl.when(not_owner)
    def _():
        red_up.middle(0)
        red_up.send_near(1)
        red_up.middle(1)

    back[...] = sc_back.finish()
    standard, inverse = spread()
    nb = back[...]
    rows_small = (
        (0, D // 128, jnp.sum(nb * standard, axis=0, keepdims=True)),
        (D // 128, D // 128, jnp.sum(nb, axis=0, keepdims=True)),
        (2 * (D // 128), HID // 128, bias_sum[...]),
    )
    small[...] = jnp.zeros_like(small)
    for first, length, row in rows_small:
        for i in range(length):
            small[first + i : first + i + 1, :] = row[:, 128 * i : 128 * (i + 1)]
    n_norm = 2 * (D // 128)
    small_over = Link(small, small_core, partner).start()
    always.append(small_over)
    scaled = nb * gain[...][None]
    back[...] = inverse * (
        scaled
        - jnp.mean(scaled, axis=1, keepdims=True)
        - standard * jnp.mean(scaled * standard, axis=1, keepdims=True)
    )
    put_back = pltpu.make_async_copy(back, out_back, local_sems.at[0])
    put_back.start()

    def small_sums():
        keep = lax.broadcasted_iota(jnp.int32, small.shape, 0) < n_norm
        small_over.got(small_core)
        small_z[z] = small[...] + jnp.where(keep, small_core[...], 0.0)
        z_links = [link(small_z.at[z], small_z.at[z], z_dev(d)) for d in range(1, 8)]
        yield
        for d, sent in zip(range(1, 8), z_links):
            sent.got(small_z.at[at_z(8 - d)])
        total = small_z[0]
        for k in range(1, 8):
            total = total + small_z[k]
        small_y[y] = total
        y_links = [link(small_y.at[y], small_y.at[y], y_dev(d)) for d in (1, 2, 3)]
        yield
        for d, sent in zip((1, 2, 3), y_links):
            sent.got(small_y.at[lax.rem(y + 4 - d, 4)])
        total = small_y[0] + small_y[1] + small_y[2] + small_y[3]
        small_x[x] = jnp.where(keep, total, small_y[y])
        x_links = [link(small_x.at[x], small_x.at[x], x_dev(d)) for d in (1, 2, 3)]
        yield
        for d, sent in zip((1, 2, 3), x_links):
            sent.got(small_x.at[lax.rem(x + 4 - d, 4)])
        small_total[0] = small_x[0] + small_x[1] + small_x[2] + small_x[3]
        last = link(small_total.at[0], small_total.at[1], partner)
        yield
        last.got(small_total.at[1])
        yield

    sums = small_sums()

    @pl.when(owner)
    def _():
        unit1.step_down(1)
        unit0.end_down()

    @pl.when(not_owner)
    def _():
        unit0.begin_up()

    sc_out.middle()
    next(sums)

    @pl.when(owner)
    def _():
        unit1.step_down(2)
        unit1.end_down()

    @pl.when(not_owner)
    def _():
        unit0.step_up()
        unit1.begin_up()
        unit0.end_up()
        unit1.step_up()
        unit1.end_up()

    first, second = unit0.spread(), unit1.spread()
    next(sums)
    next(first)
    next(second)
    next(sums)
    next(first)
    next(second)
    next(first)
    next(second)
    next(sums)
    proj[...] = sc_out.finish() + down_bias[...][None]
    put_proj = pltpu.make_async_copy(proj, out_proj, local_sems.at[1])
    put_proj.start()
    next(first)
    next(second)

    next(sums)
    put_small = pltpu.make_async_copy(small_total, out_small, local_sems.at[4])
    put_small.start()
    next(first)
    next(second)

    for link in always:
        link.sent()

    @pl.when(owner)
    def _():
        for link in when_owner:
            link.sent()

    @pl.when(jnp.logical_not(owner))
    def _():
        for link in when_relay:
            link.sent()

    for put in (put_back, put_proj, put_small, *puts):
        put.wait()
    assert count[0] <= N_LINKS


N_LINKS = 192


def on_device(patches, norm_gain, norm_bias, up_weight, up_bias, down_weight, down_bias, cotangent):
    scaling = 1.0 / math.sqrt(TOK * 256)
    vmem = pl.BlockSpec(memory_space=pltpu.VMEM)
    hbm = pl.BlockSpec(memory_space=pl.ANY)

    def V(*shape, dtype=BF):
        return pltpu.VMEM(shape, dtype)

    proj, back, mine, other, small = pl.pallas_call(
        step_kernel,
        out_shape=(
            jax.ShapeDtypeStruct((TOK, D), F32),
            jax.ShapeDtypeStruct((TOK, D), F32),
            jax.ShapeDtypeStruct((HALF, HID), BF),
            jax.ShapeDtypeStruct((HALF, HID), BF),
            jax.ShapeDtypeStruct((2, 32, 128), F32),
        ),
        in_specs=[hbm, hbm, vmem, vmem, vmem, vmem, hbm, hbm],
        out_specs=[hbm] * 5,
        scratch_shapes=[
            V(TOK, D), V(GROUP, D), V(GROUP, D), V(D, HID), V(D, HID), V(HID, dtype=F32),
            V(GROUP, HID, dtype=F32), V(GROUP, HID), V(GROUP, HID),
            V(GROUP, D), V(GROUP, D), V(4, TOK, D), V(4, TOK, D),
            V(2, 64, D), V(2, 64, D), V(2, TOK, D), V(2, TOK, D),
            V(8, CHUNK_ROWS, HID), V(8, CHUNK_ROWS, HID), V(8, CHUNK_ROWS, CHUNK_COLS), V(8, CHUNK_ROWS, CHUNK_COLS),
            V(4, CHUNK_ROWS, CHUNK_COLS), V(4, CHUNK_ROWS, HID), V(4, CHUNK_ROWS, CHUNK_COLS),
            V(4, CHUNK_ROWS, HID), V(4, CHUNK_ROWS, HID), V(4, CHUNK_ROWS, CHUNK_COLS), V(4, CHUNK_ROWS, CHUNK_COLS),
            V(8, CHUNK_ROWS, CHUNK_COLS), V(4, CHUNK_ROWS, CHUNK_COLS),
            V(4, CHUNK_ROWS, CHUNK_COLS), V(4, CHUNK_ROWS, CHUNK_COLS),
            V(8, CHUNK_ROWS, CHUNK_COLS), V(8, CHUNK_ROWS, CHUNK_COLS),
            V(TOK, D, dtype=F32), V(TOK, D, dtype=F32), V(1, HID, dtype=F32),
            V(32, 128, dtype=F32), V(32, 128, dtype=F32), V(4, 32, 128, dtype=F32),
            V(4, 32, 128, dtype=F32), V(8, 32, 128, dtype=F32), V(2, 32, 128, dtype=F32),
            pltpu.SemaphoreType.DMA((N_LINKS,)),
            pltpu.SemaphoreType.DMA((N_LINKS,)),
            pltpu.SemaphoreType.DMA((9,)),
            pltpu.SemaphoreType.DMA((32,)),
        ],
        compiler_params=pltpu.CompilerParams(
            collective_id=0, has_side_effects=True, vmem_limit_bytes=63 * 1024 * 1024
        ),
    )(
        patches, cotangent, norm_gain, norm_bias, up_bias, down_bias,
        up_weight, down_weight.T,
    )

    owner = lax.axis_index("row_0") == lax.axis_index("dp_1")

    up_grad = jnp.where(owner, other, mine).astype(F32) * scaling
    down_grad = jnp.where(owner, mine, other).astype(F32).T * scaling
    small = small * scaling
    n = D // 128
    norm_grad = small[0, : 2 * n].reshape(2, D)
    bias_grad = jnp.where(owner, small[0], small[1])[2 * n : 2 * n + HID // 128].reshape(HID)
    output = proj + patches.astype(F32)
    patch_grad = back + cotangent.astype(F32)
    return output, patch_grad, up_grad, down_grad, bias_grad, norm_grad


def solution(mesh):
    split = Mesh(
        mesh.devices.reshape(8, 2, 2, 4, mesh.shape["col"]),
        ("dp_0", "dp_1", "row_0", "row_1", "col"),
    )
    return jax.shard_map(
        on_device,
        mesh=split,
        in_specs=(
            P(DP_ROW_COL, None), P(), P(), P("col", ROW), P(ROW), P(ROW, "col"), P(), P(DP_ROW_COL, None),
        ),
        out_specs=(
            P(DP_ROW_COL, None), P(DP_ROW_COL, None), P("col", ROW), P(ROW, "col"), P(ROW), P(),
        ),
        check_vma=False,
    )
```

```python
import math

import jax
import jax.numpy as jnp
from jax import lax
from jax.experimental import pallas as pl
from jax.experimental.pallas import tpu as pltpu
from jax.sharding import Mesh
from jax.sharding import PartitionSpec as P

MESH = pl.DeviceIdType.MESH
ROW = ("row_0", "row_1")
DP_ROW_COL = ("dp_0", "dp_1", "row_0", "row_1", "col")

EPSILON = 1e-06
GELU_ROOT = 0.7978845608028654
GELU_CUBIC = 0.044715

D = 1408
HALF = 704
QUARTER = 352
HID = 768
TOK = 128
GROUP = 1024
CHUNK_ROWS, CHUNK_COLS = 176, 384
UNITS = (pl.ds(0, 96), pl.ds(96, 80))
BF = jnp.bfloat16
F32 = jnp.float32


def aligned(value, tile):
    return pl.multiple_of(value, tile)


def step_kernel(
    patches_in, cotangent_in, gain, bias, up_bias, down_bias, up, down,
    out_proj, out_back, out_mine, out_other, out_small,
    patches, normed, cot, up_all, down_all, bias_all, gelu_d, act, slope,
    part_out, part_back, core_out, core_back, far_out, far_back, near_out, near_back,
    grad_up, grad_down, swap_up, half_up, far_up, far_down, own_up, near_a, near_b, near_ua, near_ub,
    zsum, usum, z_near_a, z_near_b, mine, other,
    proj, back, bias_sum, small, small_core, small_y, small_x, small_z, small_total,
    send_sems, recv_sems, local_sems, put_sems,
):
    z, c = lax.axis_index("dp_0"), lax.axis_index("dp_1")
    xl, y, xh = lax.axis_index("row_0"), lax.axis_index("row_1"), lax.axis_index("col")
    x = xh * 2 + xl
    owner = xl == c

    def x_dev(d, swap=False):
        there = lax.rem(x + d, 4)
        place = {"row_0": lax.rem(there, 2), "col": lax.div(there, 2)}
        return {**place, "dp_1": 1 - c} if swap else place

    def y_dev(d):
        return {"row_1": lax.rem(y + d, 4)}

    def z_dev(d):
        return {"dp_0": lax.rem(z + d, 8)}

    partner = {"dp_1": 1 - c}
    peers = [partner]
    peers += [x_dev(d) for d in (1, 2, 3)] + [x_dev(d, True) for d in (1, 3)]
    peers += [y_dev(d) for d in (1, 2, 3)] + [z_dev(d) for d in range(1, 8)]
    own_rows = pl.ds(aligned((y * 2 + c) * TOK, TOK), TOK)
    own_block = pl.ds(aligned(xh * HALF, 16), HALF)
    load_patches = pltpu.make_async_copy(patches_in, patches, local_sems.at[5])
    load_cot = pltpu.make_async_copy(cotangent_in, cot.at[own_rows], local_sems.at[6])
    load_up = pltpu.make_async_copy(up, up_all.at[own_block], local_sems.at[7])
    load_down = pltpu.make_async_copy(down, down_all.at[own_block], local_sems.at[8])
    load_patches.start()
    load_cot.start()

    @pl.when(owner)
    def _():
        load_up.start()
        load_down.start()

    barrier = pltpu.get_barrier_semaphore()
    for peer in peers:
        pl.semaphore_signal(barrier, inc=1, device_id=peer, device_id_type=MESH)
    def spread():
        wide = patches[...].astype(F32)
        centred = wide - jnp.mean(wide, axis=1, keepdims=True)
        inverse = lax.rsqrt(jnp.mean(centred * centred, axis=1, keepdims=True) + EPSILON)
        return centred * inverse, inverse

    load_patches.wait()
    normed[own_rows] = (spread()[0] * gain[...][None] + bias[...][None]).astype(BF)
    load_cot.wait()
    pl.semaphore_wait(barrier, len(peers))

    count = [0]

    class Link:
        def __init__(self, src, dst, device):
            self.k = count[0]
            count[0] += 1
            self.copy = pltpu.make_async_remote_copy(
                src_ref=src, dst_ref=dst, send_sem=send_sems.at[self.k], recv_sem=recv_sems.at[self.k],
                device_id=device, device_id_type=MESH,
            )

        def start(self):
            self.copy.start()
            return self

        def sent(self):
            self.copy.wait_send()

        def got(self, dst):
            pltpu.make_async_remote_copy(
                src_ref=dst, dst_ref=dst, send_sem=send_sems.at[self.k], recv_sem=recv_sems.at[self.k],
                device_id=partner, device_id_type=MESH,
            ).wait_recv()

    always, when_owner, when_relay = [], [], []

    h_me = xh
    h_next = lax.div(lax.rem(x + 1, 4), 2)
    h_prev = lax.div(lax.rem(x + 3, 4), 2)

    lanes_x = pl.ds(aligned(lax.rem(z, 2) * CHUNK_COLS, 128), CHUNK_COLS)
    lanes_z = pl.ds(aligned((1 - lax.rem(z, 2)) * CHUNK_COLS, 128), CHUNK_COLS)

    def part(ref, h, first, lanes):
        start = aligned(h * HALF + (0 if first else QUARTER), 16)
        return ref.at[pl.ds(start, QUARTER), lanes]

    class Gather:
        def __init__(self, whole):
            def link(h, first, device):
                return Link(part(whole, h, first, lanes_x), part(whole, h, first, lanes_x), device)

            self.whole = whole
            self.a1, self.b2 = link(h_me, True, x_dev(1)), link(h_me, False, x_dev(3))
            self.b1, self.a2 = link(h_me, False, x_dev(1)), link(h_me, True, x_dev(3))
            self.ra, self.rb = link(h_prev, True, x_dev(1)), link(h_next, False, x_dev(3))
            self.oa, self.ob = link(1 - h_me, True, z_dev(1)), link(1 - h_me, False, z_dev(7))
            self.pa, self.nb = link(h_prev, True, z_dev(1)), link(h_next, False, z_dev(7))
            self.pb, self.na = link(h_prev, False, z_dev(7)), link(h_next, True, z_dev(1))
            when_owner.extend([self.a1, self.b2, self.b1, self.a2, self.oa, self.ob])
            when_relay.extend([self.ra, self.rb, self.pa, self.nb, self.pb, self.na])

        def here(self, h, first):
            return part(self.whole, h, first, lanes_x)

        def there(self, h, first):
            return part(self.whole, h, first, lanes_z)

        def begin(self):
            for link in (self.a1, self.b2, self.b1, self.a2):
                link.start()

        def relay(self):
            self.a1.got(self.here(h_prev, True))
            self.ra.start()
            self.pa.start()
            self.b2.got(self.here(h_next, False))
            self.rb.start()
            self.nb.start()

        def relay_last(self):
            self.b1.got(self.here(h_prev, False))
            self.pb.start()
            self.a2.got(self.here(h_next, True))
            self.na.start()

        def pass_on(self):
            self.ra.got(self.here(1 - h_me, True))
            self.oa.start()
            self.rb.got(self.here(1 - h_me, False))
            self.ob.start()

        def finish(self):
            @pl.when(owner)
            def _():
                self.oa.got(self.there(1 - h_me, True))
                self.ob.got(self.there(1 - h_me, False))

            @pl.when(jnp.logical_not(owner))
            def _():
                self.pa.got(self.there(h_prev, True))
                self.nb.got(self.there(h_next, False))
                self.pb.got(self.there(h_prev, False))
                self.na.got(self.there(h_next, True))

    ups, downs = Gather(up_all), Gather(down_all)
    bias_link = Link(up_bias, bias_all, x_dev(1))
    when_owner.append(bias_link)

    @pl.when(owner)
    def _():
        load_up.wait()
        ups.begin()
        bias_link.start()
        load_down.wait()
        downs.begin()
        bias_all[...] = up_bias[...]

    def slot(ref, dy, core, lo=0, rows=TOK):
        there = lax.rem(y + dy, 4)
        return ref.at[pl.ds(aligned((there * 2 + core) * TOK + lo, 16), rows)]

    class Tokens:
        def __init__(self, own, whole):
            self.whole = whole
            self.next = Link(own, slot(whole, 0, c), y_dev(1)).start()
            self.prev = Link(own, slot(whole, 0, c), y_dev(3)).start()
            self.over = Link(own, slot(whole, 0, c), partner).start()
            always.extend([self.next, self.prev, self.over])

        def relay(self):
            whole = self.whole
            self.next.got(slot(whole, 3, c))
            self.far_a = Link(slot(whole, 3, c, 0, 64), slot(whole, 3, c, 0, 64), y_dev(1)).start()
            self.over_a = Link(slot(whole, 3, c), slot(whole, 3, c), partner).start()
            self.prev.got(slot(whole, 1, c))
            self.far_b = Link(slot(whole, 1, c, 64, 64), slot(whole, 1, c, 64, 64), y_dev(3)).start()
            self.over_b = Link(slot(whole, 1, c), slot(whole, 1, c), partner).start()
            always.extend([self.far_a, self.over_a, self.far_b, self.over_b])

        def far(self):
            whole = self.whole
            self.far_a.got(slot(whole, 2, c, 0, 64))
            self.far_b.got(slot(whole, 2, c, 64, 64))
            self.over_far = Link(slot(whole, 2, c), slot(whole, 2, c), partner).start()
            always.append(self.over_far)

        def from_partner(self, dy):
            name = ("over", "over_b", "over_far", "over_a")[dy]
            getattr(self, name).got(slot(self.whole, dy, 1 - c))

    tok_n = Tokens(normed.at[own_rows], normed)
    tok_c = Tokens(cot.at[own_rows], cot)

    @pl.when(jnp.logical_not(owner))
    def _():
        ups.relay()

    tok_n.relay()

    @pl.when(owner)
    def _():
        ups.pass_on()

    @pl.when(jnp.logical_not(owner))
    def _():
        bias_link.got(bias_all)
        ups.relay_last()
        downs.relay()

    tok_c.relay()

    @pl.when(owner)
    def _():
        downs.pass_on()

    @pl.when(jnp.logical_not(owner))
    def _():
        downs.relay_last()

    def rows_of(dy):
        return pl.ds(aligned(lax.rem(y + dy, 4) * 256, 256), 256)

    def forward_block(dy):
        rows = rows_of(dy)
        v = jnp.dot(normed[rows], up_all[...], preferred_element_type=F32) + bias_all[...][None]
        inner = jnp.tanh(GELU_ROOT * (v + GELU_CUBIC * v * v * v))
        act[rows] = (0.5 * v * (1.0 + inner)).astype(BF)
        gelu_d[rows] = 0.5 * (1.0 + inner) + 0.5 * v * (1.0 - inner * inner) * GELU_ROOT * (
            1.0 + 3.0 * GELU_CUBIC * v * v
        )

    def slope_block(dy):
        rows = rows_of(dy)
        s = jnp.dot(cot[rows], down_all[...], preferred_element_type=F32) * gelu_d[rows]
        s = s.astype(BF)
        slope[rows] = s
        bias_sum[...] += jnp.sum(s.astype(F32), axis=0, keepdims=True)

    ups.finish()
    tok_n.far()
    for dy in (0, 3, 1):
        tok_n.from_partner(dy)

    @pl.loop(0, 3)
    def _(i):
        forward_block(lax.rem(i + 3, 4))

    tok_c.far()
    tok_n.from_partner(2)
    forward_block(2)

    downs.finish()
    bias_sum[...] = jnp.zeros_like(bias_sum)
    for dy in (0, 3, 1):
        tok_c.from_partner(dy)

    @pl.loop(0, 3)
    def _(i):
        slope_block(lax.rem(i + 3, 4))

    tok_c.from_partner(2)

    def outer(left, right, result):
        for lo, hi in ((0, 512), (512, 1024), (1024, D)):
            block = lax.dot_general(
                left[:, lo:hi], right[...], (((0,), (0,)), ((), ())), preferred_element_type=F32
            ).astype(BF)
            while lo < hi:
                j, r = divmod(lo, CHUNK_ROWS)
                rows = min(CHUNK_ROWS - r, hi - lo)
                result[j, r : r + rows] = block[:rows]
                block, lo = block[rows:], lo + rows

    class Reduce:
        def __init__(self, grad, far, near_a, near_b, swap):
            self.grad, self.far, self.near, self.links = grad, far, (near_a, near_b), []
            lo, hi = pl.ds(0, 2), pl.ds(2, 2)
            for rows in UNITS:
                s0 = Link(self.of(1 - h_me, True, rows), far.at[lo, rows], x_dev(1))
                s1 = Link(self.of(1 - h_me, False, rows), far.at[hi, rows], x_dev(3))
                s2 = Link(self.of(h_next, False, rows), near_a.at[hi, rows], x_dev(1, swap))
                s4 = Link(self.of(h_prev, True, rows), near_b.at[lo, rows], x_dev(3, swap))
                s3 = Link(self.of(h_next, True, rows), near_a.at[lo, rows], x_dev(1, swap))
                s5 = Link(self.of(h_prev, False, rows), near_b.at[hi, rows], x_dev(3, swap))
                when_owner.extend([s0, s1])
                when_relay.extend([s2, s4, s3, s5])
                self.links.append((s0, s1, s2, s3, s4, s5))

        def of(self, h, first, rows):
            return self.grad.at[pl.ds(h * 4 + (0 if first else 2), 2), rows]

        def send_far(self, u):
            s0, s1, _, _, _, _ = self.links[u]
            s0.start()
            s1.start()

        def send_near(self, u):
            _, _, s2, _, s4, _ = self.links[u]
            s2.start()
            s4.start()

        def middle(self, u):
            grad, far, rows = self.grad, self.far, UNITS[u]
            s0, s1, _, s3, _, s5 = self.links[u]
            for link, onward, h, first, k in ((s0, s3, h_next, True, 0), (s1, s5, h_prev, False, 2)):
                link.got(far.at[pl.ds(k, 2), rows])
                for j in (0, 1):
                    at = h * 4 + (0 if first else 2) + j
                    grad[at, rows] = (grad[at, rows].astype(F32) + far[k + j, rows].astype(F32)).astype(BF)
                onward.start()

        def finish(self, u):
            _, _, s2, s3, s4, s5 = self.links[u]
            lo, hi, rows = pl.ds(0, 2), pl.ds(2, 2), UNITS[u]
            near_a, near_b = self.near
            s2.got(near_a.at[hi, rows])
            s4.got(near_b.at[lo, rows])
            s3.got(near_a.at[lo, rows])
            s5.got(near_b.at[hi, rows])

    red_down = Reduce(grad_down, far_down, near_a, near_b, False)
    red_up = Reduce(half_up, far_up, near_ua, near_ub, True)
    own_links = []
    for rows in UNITS:
        own_links.append(Link(half_up.at[pl.ds(h_me * 4, 4), rows], own_up.at[pl.ds(0, 4), rows], partner))
    when_owner.extend(own_links)
    not_owner = jnp.logical_not(owner)

    outer(cot, act, grad_down)

    @pl.when(owner)
    def _():
        red_down.send_far(0)
        red_down.send_far(1)

    @pl.when(not_owner)
    def _():
        red_down.send_near(0)

    slope_block(2)
    outer(normed, slope, grad_up)

    swaps = []
    for rows in UNITS:
        pair = []
        for h, d in ((0, 1), (1, 7)):
            tiles = pl.ds(h * 4, 4)
            pair.append(Link(grad_up.at[tiles, rows, lanes_z], swap_up.at[tiles, rows], z_dev(d)).start())
        swaps.append(pair)
        always.extend(pair)

    def swapped(u):
        rows = UNITS[u]
        for h, swap in enumerate(swaps[u]):
            swap.got(swap_up.at[pl.ds(h * 4, 4), rows])
        for k in range(8):
            half_up[k, rows] = (grad_up[k, rows, lanes_x].astype(F32) + swap_up[k, rows].astype(F32)).astype(BF)

        @pl.when(owner)
        def _():
            own_links[u].start()
            red_up.send_far(u)

    def at_z(d):
        return lax.rem(z + d, 8)

    def add_rows(sums, k, rows, incoming):
        sums[k, rows] = (sums[k, rows].astype(F32) + incoming.astype(F32)).astype(BF)

    def link(src, dst, device):
        made = Link(src, dst, device).start()
        always.append(made)
        return made

    def held(src, dst, device, when):
        made = Link(src, dst, device)
        when.append(made)
        return made

    puts = []

    class AlongZ:
        def __init__(self, u):
            self.u, self.rows = u, UNITS[u]
            rows = self.rows
            self.head = pl.ds(rows.start, 48)
            self.tail = pl.ds(rows.start + 48, rows.size - 48)
            self.down = []
            for step in range(4):
                f, b = (self.head, self.tail) if step == 0 else (rows, rows)
                self.down.append((
                    held(zsum.at[at_z(4 - step), f], z_near_a.at[step, f], z_dev(1), when_owner),
                    held(zsum.at[at_z(4 + step), b], z_near_b.at[step, b], z_dev(7), when_owner),
                ))
            self.up = []
            for step in range(2):
                f, b = (self.head, self.tail) if step == 0 else (rows, rows)
                to, fro = lax.div(at_z(4 - 2 * step), 2), lax.div(at_z(4 + 2 * step), 2)
                self.up.append((
                    held(usum.at[to, f], z_near_a.at[step, f], z_dev(2), when_relay),
                    held(usum.at[fro, b], z_near_b.at[step, b], z_dev(6), when_relay),
                ))
            self.out = [
                held(mine.at[z, rows], mine.at[z, rows], z_dev(1), always),
                held(mine.at[z, rows], mine.at[z, rows], z_dev(7), always),
                held(mine.at[z, rows], other.at[z, rows], partner, always),
            ]

        def begin_down(self):
            red_down.finish(self.u)
            for k in range(8):
                j, lanes = k // 2, slice((k % 2) * CHUNK_COLS, (k % 2 + 1) * CHUNK_COLS)
                total = grad_down[h_me * 4 + j, self.rows, lanes].astype(F32)
                total = total + near_a[j, self.rows, lanes].astype(F32) + near_b[j, self.rows, lanes].astype(F32)
                zsum[k, self.rows] = total.astype(BF)
            for started in self.down[0]:
                started.start()

        def step_down(self, step):
            got_f, got_b = (self.head, self.tail) if step == 0 else (self.rows, self.rows)
            f, b = self.down[step]
            f.got(z_near_a.at[step, got_f])
            add_rows(zsum, at_z(3 - step), got_f, z_near_a[step, got_f])
            self.down[step + 1][0].start()
            b.got(z_near_b.at[step, got_b])
            add_rows(zsum, at_z(5 + step), got_b, z_near_b[step, got_b])
            self.down[step + 1][1].start()

        def begin_up(self):
            own_links[self.u].got(own_up.at[pl.ds(0, 4), self.rows])
            red_up.finish(self.u)
            for j in range(4):
                total = own_up[j, self.rows].astype(F32)
                total = total + near_ua[j, self.rows].astype(F32) + near_ub[j, self.rows].astype(F32)
                usum[j, self.rows] = total.astype(BF)
            for started in self.up[0]:
                started.start()

        def step_up(self):
            f, b = self.up[0]
            f.got(z_near_a.at[0, self.head])
            add_rows(usum, lax.div(at_z(2), 2), self.head, z_near_a[0, self.head])
            self.up[1][0].start()
            b.got(z_near_b.at[0, self.tail])
            add_rows(usum, lax.div(at_z(6), 2), self.tail, z_near_b[0, self.tail])
            self.up[1][1].start()

        def end(self, sums, at, links, k):
            rows = self.rows
            f, b = links
            f.got(z_near_a.at[k, rows])
            b.got(z_near_b.at[k, rows])
            mine[z, rows] = (
                sums[at, rows].astype(F32) + z_near_a[k, rows].astype(F32) + z_near_b[k, rows].astype(F32)
            ).astype(BF)
            for started in self.out:
                started.start()

        def end_down(self):
            self.end(zsum, z, self.down[3], 3)

        def end_up(self):
            self.end(usum, lax.div(z, 2), self.up[1], 1)

        def put(self, chunks, result, k):
            row = lax.div(k, 2) * CHUNK_ROWS + self.rows.start
            lane = lax.rem(k, 2) * CHUNK_COLS
            there = result.at[pl.ds(aligned(row, 16), self.rows.size), pl.ds(aligned(lane, 128), CHUNK_COLS)]
            copy = pltpu.make_async_copy(chunks.at[k, self.rows], there, put_sems.at[len(puts)])
            copy.start()
            puts.append(copy)

        def spread(self):
            rows = self.rows
            overs = [(self.out[2], z)]
            f, b = self.out[:2]
            self.put(mine, out_mine, z)

            def pass_on(k, rows, device):
                return link(mine.at[k, rows], mine.at[k, rows], device)

            def hand_over(k):
                overs.append((link(mine.at[k, rows], other.at[k, rows], partner), k))

            def take_over(count):
                for _ in range(count):
                    sent, k = overs.pop(0)
                    sent.got(other.at[k, rows])
                    self.put(other, out_other, k)

            for d in (1, 2, 3):
                f.got(mine.at[at_z(8 - d), rows])
                f = pass_on(at_z(8 - d), rows if d < 3 else self.head, z_dev(1))
                b.got(mine.at[at_z(d), rows])
                b = pass_on(at_z(d), rows if d < 3 else self.tail, z_dev(7))
                hand_over(at_z(8 - d))
                hand_over(at_z(d))
                self.put(mine, out_mine, at_z(8 - d))
                self.put(mine, out_mine, at_z(d))
                yield
            f.got(mine.at[at_z(4), self.head])
            b.got(mine.at[at_z(4), self.tail])
            hand_over(at_z(4))
            self.put(mine, out_mine, at_z(4))
            take_over(5)
            yield
            take_over(3)
            yield

    unit0, unit1 = AlongZ(0), AlongZ(1)

    def across(left, right, result):
        @pl.loop(0, GROUP // 256)
        def _(i):
            rows = pl.ds(aligned(i * 256, 256), 256)
            result[rows] = lax.dot_general(
                left[rows], right[...], (((1,), (1,)), ((), ())), preferred_element_type=F32
            ).astype(BF)

    class Scatter:
        def __init__(self, partial, core, far, near):
            self.partial, self.core, self.far, self.near = partial, core, far, near
            self.over = []
            for dy in (2, 1, 3, 0):
                there = lax.rem(y + dy, 4)
                self.over.append((dy, Link(slot(partial, dy, 1 - c), core.at[there], partner).start()))
            always.extend(link for _, link in self.over)

        def combine(self):
            partial, core = self.partial, self.core
            for dy, link in self.over:
                there = lax.rem(y + dy, 4)
                link.got(core.at[there])
                if dy == 0:
                    continue
                rows = pl.ds(aligned((there * 2 + c) * TOK, TOK), TOK)
                partial[rows] = (partial[rows].astype(F32) + core[there].astype(F32)).astype(BF)
                if dy == 2:
                    self.t0 = Link(slot(partial, 2, c, 0, 64), self.far.at[0], y_dev(1)).start()
                    self.t1 = Link(slot(partial, 2, c, 64, 64), self.far.at[1], y_dev(3)).start()
                elif dy == 1:
                    self.t2 = Link(slot(partial, 1, c, 64, 64), self.near.at[0, pl.ds(64, 64)], y_dev(1)).start()
                else:
                    self.t3 = Link(slot(partial, 3, c, 0, 64), self.near.at[1, pl.ds(0, 64)], y_dev(3)).start()
            always.extend([self.t0, self.t1, self.t2, self.t3])

        def middle(self):
            partial, far = self.partial, self.far
            for dy, lo, k, link in ((1, 0, 0, self.t0), (3, 64, 1, self.t1)):
                link.got(far.at[k])
                there = lax.rem(y + dy, 4)
                rows = pl.ds(aligned((there * 2 + c) * TOK + lo, 16), 64)
                partial[rows] = (partial[rows].astype(F32) + far[k].astype(F32)).astype(BF)
                onward = Link(slot(partial, dy, c, lo, 64), self.near.at[k, pl.ds(lo, 64)], y_dev(dy)).start()
                always.append(onward)
                if k == 0:
                    self.t4 = onward
                else:
                    self.t5 = onward

        def finish(self):
            near = self.near
            self.t2.got(near.at[0, pl.ds(64, 64)])
            self.t3.got(near.at[1, pl.ds(0, 64)])
            self.t4.got(near.at[0, pl.ds(0, 64)])
            self.t5.got(near.at[1, pl.ds(64, 64)])
            own = self.partial[own_rows].astype(F32) + self.core[y].astype(F32)
            return own + near[0].astype(F32) + near[1].astype(F32)

    across(slope, up_all, part_back)
    sc_back = Scatter(part_back, core_back, far_back, near_back)


    @pl.when(not_owner)
    def _():
        red_down.middle(0)
        red_down.send_near(1)

    across(act, down_all, part_out)
    sc_out = Scatter(part_out, core_out, far_out, near_out)

    swapped(0)

    @pl.when(not_owner)
    def _():
        red_up.send_near(0)

    sc_back.combine()

    @pl.when(not_owner)
    def _():
        red_down.middle(1)

    swapped(1)

    @pl.when(owner)
    def _():
        unit0.begin_down()

    sc_back.middle()

    @pl.when(owner)
    def _():
        unit0.step_down(0)

    sc_out.combine()

    @pl.when(owner)
    def _():
        unit1.begin_down()
        unit0.step_down(1)
        unit1.step_down(0)
        unit0.step_down(2)

    @pl.when(not_owner)
    def _():
        red_up.middle(0)
        red_up.send_near(1)
        red_up.middle(1)

    back[...] = sc_back.finish()
    standard, inverse = spread()
    nb = back[...]
    rows_small = (
        (0, D // 128, jnp.sum(nb * standard, axis=0, keepdims=True)),
        (D // 128, D // 128, jnp.sum(nb, axis=0, keepdims=True)),
        (2 * (D // 128), HID // 128, bias_sum[...]),
    )
    small[...] = jnp.zeros_like(small)
    for first, length, row in rows_small:
        for i in range(length):
            small[first + i : first + i + 1, :] = row[:, 128 * i : 128 * (i + 1)]
    n_norm = 2 * (D // 128)
    small_over = Link(small, small_core, partner).start()
    always.append(small_over)
    scaled = nb * gain[...][None]
    back[...] = inverse * (
        scaled
        - jnp.mean(scaled, axis=1, keepdims=True)
        - standard * jnp.mean(scaled * standard, axis=1, keepdims=True)
    )
    put_back = pltpu.make_async_copy(back, out_back, local_sems.at[0])
    put_back.start()

    def small_sums():
        keep = lax.broadcasted_iota(jnp.int32, small.shape, 0) < n_norm
        small_over.got(small_core)
        small_z[z] = small[...] + jnp.where(keep, small_core[...], 0.0)
        z_links = [link(small_z.at[z], small_z.at[z], z_dev(d)) for d in range(1, 8)]
        yield
        for d, sent in zip(range(1, 8), z_links):
            sent.got(small_z.at[at_z(8 - d)])
        total = small_z[0]
        for k in range(1, 8):
            total = total + small_z[k]
        small_y[y] = total
        y_links = [link(small_y.at[y], small_y.at[y], y_dev(d)) for d in (1, 2, 3)]
        yield
        for d, sent in zip((1, 2, 3), y_links):
            sent.got(small_y.at[lax.rem(y + 4 - d, 4)])
        total = small_y[0] + small_y[1] + small_y[2] + small_y[3]
        small_x[x] = jnp.where(keep, total, small_y[y])
        x_links = [link(small_x.at[x], small_x.at[x], x_dev(d)) for d in (1, 2, 3)]
        yield
        for d, sent in zip((1, 2, 3), x_links):
            sent.got(small_x.at[lax.rem(x + 4 - d, 4)])
        small_total[0] = small_x[0] + small_x[1] + small_x[2] + small_x[3]
        last = link(small_total.at[0], small_total.at[1], partner)
        yield
        last.got(small_total.at[1])
        yield

    sums = small_sums()

    @pl.when(owner)
    def _():
        unit1.step_down(1)
        unit0.end_down()

    @pl.when(not_owner)
    def _():
        unit0.begin_up()

    sc_out.middle()

    @pl.when(owner)
    def _():
        unit1.step_down(2)
        unit1.end_down()

    @pl.when(not_owner)
    def _():
        unit1.begin_up()
        unit0.step_up()
        unit1.step_up()
        unit0.end_up()
        unit1.end_up()

    first, second = unit0.spread(), unit1.spread()
    next(sums)
    next(first)
    next(second)
    next(sums)
    next(first)
    next(second)
    next(sums)
    next(first)
    next(second)
    next(sums)
    proj[...] = sc_out.finish() + down_bias[...][None]
    put_proj = pltpu.make_async_copy(proj, out_proj, local_sems.at[1])
    put_proj.start()
    next(first)
    next(second)

    next(sums)
    put_small = pltpu.make_async_copy(small_total, out_small, local_sems.at[4])
    put_small.start()
    next(first)
    next(second)

    for link in always:
        link.sent()

    @pl.when(owner)
    def _():
        for link in when_owner:
            link.sent()

    @pl.when(jnp.logical_not(owner))
    def _():
        for link in when_relay:
            link.sent()

    for put in (put_back, put_proj, put_small, *puts):
        put.wait()
    assert count[0] == N_LINKS, count[0]


N_LINKS = 162


def on_device(patches, norm_gain, norm_bias, up_weight, up_bias, down_weight, down_bias, cotangent):
    scaling = 1.0 / math.sqrt(TOK * 256)
    vmem = pl.BlockSpec(memory_space=pltpu.VMEM)
    hbm = pl.BlockSpec(memory_space=pl.ANY)

    def V(*shape, dtype=BF):
        return pltpu.VMEM(shape, dtype)

    proj, back, mine, other, small = pl.pallas_call(
        step_kernel,
        out_shape=(
            jax.ShapeDtypeStruct((TOK, D), F32),
            jax.ShapeDtypeStruct((TOK, D), F32),
            jax.ShapeDtypeStruct((HALF, HID), BF),
            jax.ShapeDtypeStruct((HALF, HID), BF),
            jax.ShapeDtypeStruct((2, 32, 128), F32),
        ),
        in_specs=[hbm, hbm, vmem, vmem, vmem, vmem, hbm, hbm],
        out_specs=[hbm] * 5,
        scratch_shapes=[
            V(TOK, D), V(GROUP, D), V(GROUP, D), V(D, HID), V(D, HID), V(HID, dtype=F32),
            V(GROUP, HID, dtype=F32), V(GROUP, HID), V(GROUP, HID),
            V(GROUP, D), V(GROUP, D), V(4, TOK, D), V(4, TOK, D),
            V(2, 64, D), V(2, 64, D), V(2, TOK, D), V(2, TOK, D),
            V(8, CHUNK_ROWS, HID), V(8, CHUNK_ROWS, HID), V(8, CHUNK_ROWS, CHUNK_COLS), V(8, CHUNK_ROWS, CHUNK_COLS),
            V(4, CHUNK_ROWS, CHUNK_COLS), V(4, CHUNK_ROWS, HID), V(4, CHUNK_ROWS, CHUNK_COLS),
            V(4, CHUNK_ROWS, HID), V(4, CHUNK_ROWS, HID), V(4, CHUNK_ROWS, CHUNK_COLS), V(4, CHUNK_ROWS, CHUNK_COLS),
            V(8, CHUNK_ROWS, CHUNK_COLS), V(4, CHUNK_ROWS, CHUNK_COLS),
            V(4, CHUNK_ROWS, CHUNK_COLS), V(4, CHUNK_ROWS, CHUNK_COLS),
            V(8, CHUNK_ROWS, CHUNK_COLS), V(8, CHUNK_ROWS, CHUNK_COLS),
            V(TOK, D, dtype=F32), V(TOK, D, dtype=F32), V(1, HID, dtype=F32),
            V(32, 128, dtype=F32), V(32, 128, dtype=F32), V(4, 32, 128, dtype=F32),
            V(4, 32, 128, dtype=F32), V(8, 32, 128, dtype=F32), V(2, 32, 128, dtype=F32),
            pltpu.SemaphoreType.DMA((N_LINKS,)),
            pltpu.SemaphoreType.DMA((N_LINKS,)),
            pltpu.SemaphoreType.DMA((9,)),
            pltpu.SemaphoreType.DMA((32,)),
        ],
        compiler_params=pltpu.CompilerParams(
            collective_id=0, has_side_effects=True, vmem_limit_bytes=63 * 1024 * 1024
        ),
    )(
        patches, cotangent, norm_gain, norm_bias, up_bias, down_bias,
        up_weight, down_weight.T,
    )

    owner = lax.axis_index("row_0") == lax.axis_index("dp_1")

    up_grad = jnp.where(owner, other, mine).astype(F32) * scaling
    down_grad = jnp.where(owner, mine, other).astype(F32).T * scaling
    small = small * scaling
    n = D // 128
    norm_grad = small[0, : 2 * n].reshape(2, D)
    bias_grad = jnp.where(owner, small[0], small[1])[2 * n : 2 * n + HID // 128].reshape(HID)
    output = proj + patches.astype(F32)
    patch_grad = back + cotangent.astype(F32)
    return output, patch_grad, up_grad, down_grad, bias_grad, norm_grad


def solution(mesh):
    split = Mesh(
        mesh.devices.reshape(8, 2, 2, 4, mesh.shape["col"]),
        ("dp_0", "dp_1", "row_0", "row_1", "col"),
    )
    return jax.shard_map(
        on_device,
        mesh=split,
        in_specs=(
            P(DP_ROW_COL, None), P(), P(), P("col", ROW), P(ROW), P(ROW, "col"), P(), P(DP_ROW_COL, None),
        ),
        out_specs=(
            P(DP_ROW_COL, None), P(DP_ROW_COL, None), P("col", ROW), P(ROW, "col"), P(ROW), P(),
        ),
        check_vma=False,
    )
```
